512 devices in a mesh: dp: 64 (over x, z, y_hi), mp: 8 (over y_lo, core).
Axes of the slice: x: 4, y: 8 (y_hi: 2, y_lo: 4; y = y_hi * 4 + y_lo), z: 8, core: 2. Of those that a mesh axis runs over, the one named last changes fastest.
Arguments:
- gradient: bfloat16 [8, 32, 512, 512], P('mp', None, 'dp'), may hold values from -54 to 54
- owners: int32 [8, 32], P('mp'), may hold values from 0 to 63, as said below
- left_stats: float32 [8, 64, 512, 512], P('mp', 'dp'), may hold values from -0.2 to 20.2
- right_stats: float32 [8, 64, 512, 512], P('mp', 'dp'), may hold values from -0.2 to 20.2
- left_roots_old: bfloat16 [8, 64, 512, 512], P('mp', 'dp'), may hold values from -0.1 to 1.5
- right_roots_old: bfloat16 [8, 64, 512, 512], P('mp', 'dp'), may hold values from -0.1 to 1.5
Outputs:
- update: bfloat16 [8, 32, 512, 512], P('mp', None, 'dp')
- left_roots: bfloat16 [8, 64, 512, 512], P('mp', 'dp')
- right_roots: bfloat16 [8, 64, 512, 512], P('mp', 'dp')
The draws below stay inside these ranges and needn't reach their ends.
Inputs may be any that keep to these rules, and one draw needn't show every extreme that they name: In each row the 32 owners are distinct. Owner o holds a block of row m exactly when owner (o + 32) mod 64 of row m holds none, and exactly when owner o of row (m + 4) mod 8 holds none.
All inputs are finite; a program needn't handle non-finite values.
Results may differ from the reference program's by a relative error of at most 0.0067.
Values may be sent and summed in bfloat16 or wider, within the bound.
No kernel may reach another device: no remote copies, remote signals or barrier semaphores. Data moves between devices by JAX's collectives and lax.ppermute only.
A program may use at most 64 MiB of HBM per device.

```python
import math
import jax
import jax.numpy as jnp
from jax import lax

BLOCK = 512
ITERS = 2
NB = 32
N_DP = 64
N_MP = 8


def draw_gradient(key, part):
    key_noise, key_rows, key_cols = jax.random.split(key, 3)
    full_shape = (N_MP, NB, BLOCK, BLOCK)
    random_part = jax.random.truncated_normal(key_noise, -4.0, 4.0, full_shape, jnp.float32)
    upper_scale = 3.16
    row_scale = jnp.exp(jax.random.uniform(key_rows, (N_MP, NB, BLOCK, 1), jnp.float32, 0.0, math.log(upper_scale)))
    col_scale = jnp.exp(jax.random.uniform(key_cols, (N_MP, NB, 1, BLOCK), jnp.float32, 0.0, math.log(upper_scale)))
    rise_scale = (3.0 ** (jnp.arange(N_MP, dtype=jnp.float32) / (N_MP - 1))).reshape(N_MP, 1, 1, 1)
    return (0.25 * random_part * row_scale * col_scale * rise_scale).astype(jnp.bfloat16)


def draw_owners(key, part):
    half_dp = N_DP // 2
    half_mp = N_MP // 2
    key_bits, key_order = jax.random.split(jax.random.fold_in(key, 7))
    corner = jax.random.randint(key_bits, (half_mp, half_dp), 0, 2).astype(jnp.int32)
    corner_rows = jnp.concatenate([corner, corner], axis=0)
    upper_half = (jnp.arange(N_MP, dtype=jnp.int32) >= half_mp).astype(jnp.int32)[:, None]
    lower_busy = jnp.bitwise_xor(corner_rows, upper_half)
    busy_owner = jnp.arange(half_dp, dtype=jnp.int32)[None, :] + half_dp * (1 - lower_busy)
    scores = jax.random.randint(key_order, (N_MP, half_dp), 0, 1 << 20).astype(jnp.int32) * half_dp + jnp.arange(half_dp, dtype=jnp.int32)[None, :]
    ranking = jnp.argsort(scores, axis=1)
    return jnp.take_along_axis(busy_owner, ranking, axis=1).astype(jnp.int32)


def symmetric_draw(key, lower, upper, spread):
    key_diag, key_off = jax.random.split(key)
    diag_values = jnp.exp(jax.random.uniform(key_diag, (N_MP, N_DP, BLOCK), jnp.float32, math.log(lower), math.log(upper)))
    off_raw = jax.random.truncated_normal(key_off, -4.0, 4.0, (N_MP, N_DP, BLOCK, BLOCK), jnp.float32)
    off_sym = (off_raw + jnp.swapaxes(off_raw, 2, 3)) * (spread * lower / math.sqrt(BLOCK))
    return off_sym + diag_values[..., None] * jnp.eye(BLOCK, dtype=jnp.float32)


def draw_left_stats(key, part):
    return symmetric_draw(jax.random.fold_in(key, 11), 1.0, 10.0, 0.2)


def draw_right_stats(key, part):
    return symmetric_draw(jax.random.fold_in(key, 13), 1.0, 10.0, 0.2)


def draw_left_roots_old(key, part):
    return symmetric_draw(jax.random.fold_in(key, 17), 0.4, 1.2, 0.4).astype(jnp.bfloat16)


def draw_right_roots_old(key, part):
    return symmetric_draw(jax.random.fold_in(key, 19), 0.4, 1.2, 0.4).astype(jnp.bfloat16)


def setup_inputs(seed: int = 0) -> dict:
    streams_of = jax.random.split(jax.random.key(seed), 7)
    gradient = draw_gradient(jax.random.fold_in(streams_of[6], 71), 0)
    owners = draw_owners(jax.random.fold_in(streams_of[6], 71), 0)
    left_stats = draw_left_stats(jax.random.fold_in(streams_of[6], 71), 0)
    right_stats = draw_right_stats(jax.random.fold_in(streams_of[6], 71), 0)
    left_roots_old = draw_left_roots_old(jax.random.fold_in(streams_of[6], 71), 0)
    right_roots_old = draw_right_roots_old(jax.random.fold_in(streams_of[6], 71), 0)
    return {"gradient": gradient, "owners": owners, "left_stats": left_stats, "right_stats": right_stats, "left_roots_old": left_roots_old, "right_roots_old": right_roots_old}


stat_decay = 0.9
ridge_term = 0.001
tiny_term = 1e-06

def newton_root(statistic):
    dimension = statistic.shape[0]
    identity = jnp.eye(dimension, dtype=jnp.float32)
    shifted = statistic + ridge_term * identity
    norm_scale = jnp.sqrt(jnp.sum(shifted * shifted) + tiny_term)
    matrix = shifted / norm_scale
    iterate = identity
    for iteration in range(ITERS):
        factor = ((5.0 * identity - matrix) / 4.0).astype(jnp.bfloat16)
        if iteration == 0:
            iterate = norm_scale ** (-0.25) * lax.optimization_barrier(factor).astype(jnp.float32)
        else:
            iterate = jnp.dot(iterate.astype(jnp.bfloat16), factor, preferred_element_type=jnp.float32)
        if iteration + 1 < ITERS:
            factor_two = jnp.dot(factor, factor, preferred_element_type=jnp.float32).astype(jnp.bfloat16)
            factor_four = jnp.dot(factor_two, factor_two, preferred_element_type=jnp.float32).astype(jnp.bfloat16)
            matrix = jnp.dot(factor_four, matrix.astype(jnp.bfloat16), preferred_element_type=jnp.float32)
    return iterate.astype(jnp.bfloat16)

def reference(gradient, owners, left_stats, right_stats, left_roots_old, right_roots_old):
    shard_grid = jnp.broadcast_to(jnp.arange(N_MP, dtype=jnp.int32)[:, None], (N_MP, NB))
    block_grid = jnp.broadcast_to(jnp.arange(NB, dtype=jnp.int32)[None, :], (N_MP, NB))
    index_pairs = jnp.stack([shard_grid.reshape(-1), block_grid.reshape(-1)], axis=1)

    def per_block(indices):
        shard_id = indices[0]
        block_id = indices[1]
        owner_id = owners[shard_id, block_id]
        grad_block = gradient[shard_id, block_id]
        left_gram = jnp.dot(grad_block, grad_block.T, preferred_element_type=jnp.float32)
        right_gram = jnp.dot(grad_block.T, grad_block, preferred_element_type=jnp.float32)
        left_new = stat_decay * left_stats[shard_id, owner_id] + left_gram / BLOCK
        right_new = stat_decay * right_stats[shard_id, owner_id] + right_gram / BLOCK
        shaded = jnp.dot(grad_block, right_roots_old[shard_id, owner_id], preferred_element_type=jnp.float32).astype(jnp.bfloat16)
        direction = jnp.dot(left_roots_old[shard_id, owner_id], shaded, preferred_element_type=jnp.float32).astype(jnp.bfloat16)
        grad_square = jnp.sum(jnp.square(grad_block.astype(jnp.float32)))
        dir_square = jnp.sum(jnp.square(direction.astype(jnp.float32)))
        return (direction, grad_square, dir_square, newton_root(left_new), newton_root(right_new))
    directions, grad_squares, dir_squares, left_new_roots, right_new_roots = lax.map(per_block, index_pairs)
    grad_totals = lax.optimization_barrier(jnp.sum(grad_squares.reshape(N_MP, NB), axis=0))
    dir_totals = lax.optimization_barrier(jnp.sum(dir_squares.reshape(N_MP, NB), axis=0))
    graft_scale = jnp.sqrt(grad_totals / (dir_totals + tiny_term))
    update = (graft_scale[None, :, None, None] * directions.reshape(N_MP, NB, BLOCK, BLOCK).astype(jnp.float32)).astype(jnp.bfloat16)
    left_roots = jnp.zeros((N_MP, N_DP, BLOCK, BLOCK), jnp.bfloat16).at[shard_grid, owners].set(left_new_roots.reshape(N_MP, NB, BLOCK, BLOCK))
    right_roots = jnp.zeros((N_MP, N_DP, BLOCK, BLOCK), jnp.bfloat16).at[shard_grid, owners].set(right_new_roots.reshape(N_MP, NB, BLOCK, BLOCK))
    return (update, left_roots, right_roots)
```

```python
import jax
import jax.numpy as jnp
from jax import lax
from jax.experimental import pallas as pl
from jax.experimental.pallas import tpu as pltpu
from jax.sharding import Mesh
from jax.sharding import PartitionSpec as P

ITERS = 2
DP = ("dp_0h", "dp_0l", "dp_1", "dp_2")
MP = ("mp_0", "mp_1")
NEAR = ("dp_0h", "mp_0", "mp_1")
LANES = 128
MIB = 1024 * 1024


stat_decay = 0.9
ridge_term = 0.001
tiny_term = 1e-06

SMEM = pl.BlockSpec(memory_space=pltpu.SMEM)
VMEM = pl.BlockSpec(memory_space=pltpu.VMEM)


def params(mib):
    return pltpu.CompilerParams(vmem_limit_bytes=mib * MIB)


def partner_of(owner, dp_count):
    half = dp_count // 2
    return jnp.where(owner < half, owner + half, owner - half)


def place_blocks(owners, blocks, dp_count):
    blocks_here, row_count, width = blocks.shape

    def body(owner_ref, block_ref, slot_ref):
        for j in range(blocks_here):
            owner = owner_ref[0, j]
            rows = block_ref[j]
            slot_ref[owner] = rows
            slot_ref[partner_of(owner, dp_count)] = rows

    return pl.pallas_call(
        body,
        out_shape=jax.ShapeDtypeStruct((dp_count, row_count, width), blocks.dtype),
        in_specs=[SMEM, VMEM],
        out_specs=VMEM,
        compiler_params=params(4),
        name="place_blocks",
    )(owners, blocks)


def precondition(busy, masks, grad_block, left, right, near_count):
    def body(busy_ref, mask_ref, grad_ref, left_ref, right_ref, dir_ref, norm_ref):
        @pl.when(busy_ref[0] == 1)
        def _():
            grad = grad_ref[...]
            shaded = jnp.dot(grad, right_ref[...], preferred_element_type=jnp.float32)
            direction = jnp.dot(
                left_ref[...], shaded.astype(jnp.bfloat16), preferred_element_type=jnp.float32
            ).astype(jnp.bfloat16)
            dir_ref[...] = direction
            wide = grad.astype(jnp.float32)
            grad_square = jnp.sum(wide * wide, keepdims=True)
            wide = direction.astype(jnp.float32)
            dir_square = jnp.sum(wide * wide, keepdims=True)
            row = mask_ref[0:1] * grad_square + mask_ref[1:2] * dir_square
            norm_ref[...] = jnp.broadcast_to(row[None], norm_ref.shape)

        @pl.when(busy_ref[0] == 0)
        def _():
            norm_ref[...] = jnp.zeros_like(norm_ref)

    return pl.pallas_call(
        body,
        out_shape=(
            jax.ShapeDtypeStruct(grad_block.shape, jnp.bfloat16),
            jax.ShapeDtypeStruct((near_count, 1, LANES), jnp.float32),
        ),
        in_specs=[SMEM, VMEM, VMEM, VMEM, VMEM],
        out_specs=(VMEM, VMEM),
        compiler_params=params(12),
        name="precondition",
    )(busy, masks, grad_block, left, right)


def add_norms(busy, near_norms, slots):
    def body(busy_ref, near_ref, slot_ref, out_ref, rows_ref, sem):
        del slot_ref

        @pl.when(busy_ref[0] == 0)
        def _():
            total = jnp.sum(near_ref[...], axis=0)
            high = total.astype(jnp.bfloat16).astype(jnp.float32)
            rest = total - high
            middle = rest.astype(jnp.bfloat16).astype(jnp.float32)
            low = rest - middle
            row = lax.broadcasted_iota(jnp.int32, rows_ref.shape[1:], 0)
            shape = rows_ref.shape[1:]
            packed = jnp.where(
                row == 0,
                jnp.broadcast_to(high, shape),
                jnp.where(
                    row == 1,
                    jnp.broadcast_to(middle, shape),
                    jnp.where(row == 2, jnp.broadcast_to(low, shape), 0.0),
                ),
            ).astype(jnp.bfloat16)
            rows_ref[...] = jnp.broadcast_to(packed[None], rows_ref.shape)
            copy = pltpu.make_async_copy(rows_ref, out_ref.at[:, :, 0:LANES], sem)
            copy.start()
            copy.wait()

    dp_count, row_count, _ = slots.shape
    return pl.pallas_call(
        body,
        out_shape=jax.ShapeDtypeStruct(slots.shape, slots.dtype),
        in_specs=[SMEM, VMEM, pl.BlockSpec(memory_space=pl.ANY)],
        out_specs=pl.BlockSpec(memory_space=pl.ANY),
        scratch_shapes=[
            pltpu.VMEM((dp_count, row_count, LANES), slots.dtype),
            pltpu.SemaphoreType.DMA,
        ],
        input_output_aliases={2: 0},
        compiler_params=params(4),
        name="add_norms",
    )(busy, near_norms, slots)


def scale_blocks(owners, slots):
    blocks_here = owners.shape[1]
    dp_count, row_count, width = slots.shape

    def body(owner_ref, slot_ref, out_ref):
        norms = jnp.zeros((row_count, LANES), jnp.float32)
        for j in range(blocks_here):
            idle = partner_of(owner_ref[0, j], dp_count)
            norms = norms + slot_ref[idle, :, 0:LANES].astype(jnp.float32)
        totals = norms[0:1] + (norms[1:2] + norms[2:3])
        columns = jnp.broadcast_to(totals, (LANES, LANES)).T
        ratio = jnp.sqrt(
            columns[:blocks_here] / (columns[blocks_here : 2 * blocks_here] + tiny_term)
        )
        for j in range(blocks_here):
            owner = owner_ref[0, j]
            scale = jnp.broadcast_to(ratio[j : j + 1], (row_count, LANES))
            for c in range(width // LANES):
                at = slice(c * LANES, (c + 1) * LANES)
                rows = slot_ref[owner, :, at].astype(jnp.float32)
                out_ref[j, :, at] = (scale * rows).astype(out_ref.dtype)

    return pl.pallas_call(
        body,
        out_shape=jax.ShapeDtypeStruct((blocks_here, row_count, width), slots.dtype),
        in_specs=[SMEM, VMEM],
        out_specs=VMEM,
        compiler_params=params(4),
        name="scale_blocks",
    )(owners, slots)


def refresh(busy, grad_block, left_stats, right_stats):
    order = grad_block.shape[0]
    strip = 64

    def body(busy_ref, grad_ref, left_ref, right_ref, left_out, right_out, wide, low, first):
        def one(stat_ref, out_ref, dims):
            grad = grad_ref[...]
            wide[...] = lax.dot_general(grad, grad, dims, preferred_element_type=jnp.float32)

            def shift(i, total):
                at = pl.ds(i * strip, strip)
                on_diagonal = lax.broadcasted_iota(
                    jnp.int32, (strip, order), 1
                ) == i * strip + lax.broadcasted_iota(jnp.int32, (strip, order), 0)
                shifted = stat_decay * stat_ref[at] + wide[at] / order
                shifted = shifted + jnp.where(on_diagonal, ridge_term, 0.0)
                wide[at] = shifted
                return total + jnp.sum(
                    (shifted * shifted).reshape(strip // 8, 8, order), axis=0
                )

            squares = lax.fori_loop(
                0, order // strip, shift, jnp.zeros((8, order), jnp.float32)
            )
            scale = jnp.sqrt(jnp.sum(squares, keepdims=True) + tiny_term)
            start = 1.0 / jnp.sqrt(jnp.sqrt(scale))

            def begin(i, carry):
                at = pl.ds(i * strip, strip)
                on_diagonal = lax.broadcasted_iota(
                    jnp.int32, (strip, order), 1
                ) == i * strip + lax.broadcasted_iota(jnp.int32, (strip, order), 0)
                matrix = wide[at] / scale
                factor = ((jnp.where(on_diagonal, 5.0, 0.0) - matrix) / 4.0).astype(jnp.bfloat16)
                low[0, at] = matrix.astype(jnp.bfloat16)
                low[1, at] = factor
                first[at] = (start * factor.astype(jnp.float32)).astype(jnp.bfloat16)
                return carry

            lax.fori_loop(0, order // strip, begin, 0)

            def dot(a, b):
                return jnp.dot(a, b, preferred_element_type=jnp.float32)

            low[2] = dot(low[1], low[1]).astype(jnp.bfloat16)
            low[1] = dot(low[2], low[2]).astype(jnp.bfloat16)
            wide[...] = dot(low[1], low[0])

            def again(i, carry):
                at = pl.ds(i * strip, strip)
                on_diagonal = lax.broadcasted_iota(
                    jnp.int32, (strip, order), 1
                ) == i * strip + lax.broadcasted_iota(jnp.int32, (strip, order), 0)
                low[2, at] = ((jnp.where(on_diagonal, 5.0, 0.0) - wide[at]) / 4.0).astype(
                    jnp.bfloat16
                )
                return carry

            lax.fori_loop(0, order // strip, again, 0)
            out_ref[...] = dot(first[...], low[2]).astype(jnp.bfloat16)

        @pl.when(busy_ref[0] == 1)
        def _():
            one(left_ref, left_out, (((1,), (1,)), ((), ())))
            one(right_ref, right_out, (((0,), (0,)), ((), ())))

        @pl.when(busy_ref[0] == 0)
        def _():
            left_out[...] = jnp.zeros_like(left_out)
            right_out[...] = jnp.zeros_like(right_out)

    root = jax.ShapeDtypeStruct((order, order), jnp.bfloat16)
    return pl.pallas_call(
        body,
        out_shape=(root, root),
        in_specs=[SMEM, VMEM, VMEM, VMEM],
        out_specs=(VMEM, VMEM),
        scratch_shapes=[
            pltpu.VMEM((order, order), jnp.float32),
            pltpu.VMEM((3, order, order), jnp.bfloat16),
            pltpu.VMEM((order, order), jnp.bfloat16),
        ],
        compiler_params=params(24),
        name="refresh",
    )(busy, grad_block, left_stats, right_stats)


def shards(gradient, owners, left_stats, right_stats, left_roots_old, right_roots_old):
    dp_count = lax.axis_size(DP)
    near_count = lax.axis_size(NEAR)
    my_index = lax.axis_index(DP)
    blocks_here = gradient.shape[1]
    row_count = gradient.shape[2]
    block_width = gradient.shape[3]
    is_mine = owners[0] == my_index
    busy = jnp.any(is_mine).astype(jnp.int32).reshape(1)
    mine = is_mine.astype(jnp.float32)
    masks = jnp.stack(
        [
            jnp.pad(mine, (0, LANES - blocks_here)),
            jnp.pad(mine, (blocks_here, LANES - 2 * blocks_here)),
        ]
    )
    outgoing = place_blocks(owners, gradient[0], dp_count)
    arrived = lax.all_to_all(outgoing, DP, split_axis=0, concat_axis=0, tiled=True)
    grad_block = arrived.reshape(dp_count * row_count, block_width)
    direction, norms = precondition(
        busy, masks, grad_block, left_roots_old[0, 0], right_roots_old[0, 0], near_count
    )
    near_norms = lax.all_to_all(norms, NEAR, split_axis=0, concat_axis=0, tiled=True)
    slots = add_norms(busy, near_norms, direction.reshape(dp_count, row_count, block_width))
    returned = lax.all_to_all(slots, DP, split_axis=0, concat_axis=0, tiled=True)
    left_root, right_root = refresh(busy, grad_block, left_stats[0, 0], right_stats[0, 0])
    update = scale_blocks(owners, returned)[None]
    return (update, left_root[None, None], right_root[None, None])


def solution(mesh):
    finer = Mesh(
        mesh.devices.reshape(2, 2, 8, 2, 4, 2),
        ("dp_0h", "dp_0l", "dp_1", "dp_2", "mp_0", "mp_1"),
    )
    placed = (
        P(MP, None, DP, None),
        P(MP, None),
        P(MP, DP, None, None),
        P(MP, DP, None, None),
        P(MP, DP, None, None),
        P(MP, DP, None, None),
    )
    return jax.shard_map(
        shards,
        mesh=finer,
        in_specs=placed,
        out_specs=(P(MP, None, DP, None), P(MP, DP, None, None), P(MP, DP, None, None)),
        check_vma=False,
    )
```

```python
import jax
import jax.numpy as jnp
from jax import lax
from jax.experimental import pallas as pl
from jax.experimental.pallas import tpu as pltpu
from jax.sharding import Mesh
from jax.sharding import PartitionSpec as P

ITERS = 2
DP = ("dp_0h", "dp_0l", "dp_1", "dp_2")
MP = ("mp_0", "mp_1")
NEAR = ("dp_0h", "mp_0", "mp_1")
PAIRS = ("dp_0l", "dp_1", "dp_2")
LANES = 128
MIB = 1024 * 1024


stat_decay = 0.9
ridge_term = 0.001
tiny_term = 1e-06

SMEM = pl.BlockSpec(memory_space=pltpu.SMEM)
VMEM = pl.BlockSpec(memory_space=pltpu.VMEM)
ANY = pl.BlockSpec(memory_space=pl.ANY)


def params(mib):
    return pltpu.CompilerParams(vmem_limit_bytes=mib * MIB)


def partner_of(owner, dp_count):
    half = dp_count // 2
    return jnp.where(owner < half, owner + half, owner - half)


def place_blocks(owners, blocks, dp_count):
    blocks_here, row_count, width = blocks.shape

    def body(owner_ref, block_ref, slot_ref, sems):
        copies = []
        for j in range(blocks_here):
            owner = owner_ref[0, j]
            for k, slot in enumerate((owner, partner_of(owner, dp_count))):
                copy = pltpu.make_async_copy(block_ref.at[j], slot_ref.at[slot], sems.at[2 * j + k])
                copy.start()
                copies.append(copy)
        for copy in copies:
            copy.wait()

    return pl.pallas_call(
        body,
        out_shape=jax.ShapeDtypeStruct((dp_count, row_count, width), blocks.dtype),
        in_specs=[SMEM, ANY],
        out_specs=ANY,
        scratch_shapes=[pltpu.SemaphoreType.DMA((2 * blocks_here,))],
        name="place_blocks",
    )(owners, blocks)


def precondition(place, masks, grad_block, left, right, near_count, row_count):
    order = grad_block.shape[0]
    half = order // 2
    slots = half // row_count

    def body(place_ref, mask_ref, grad_ref, left_ref, right_ref, stay_ref, pass_ref, norm_ref):
        @pl.when(place_ref[0] == 1)
        def _():
            grad = grad_ref[...]
            shaded = jnp.dot(grad, right_ref[...], preferred_element_type=jnp.float32)
            shaded = shaded.astype(jnp.bfloat16)

            def rows_of(which):
                at = pl.ds(pl.multiple_of(which * half, half), half)
                rows = jnp.dot(left_ref[at], shaded, preferred_element_type=jnp.float32)
                return rows.astype(jnp.bfloat16)

            passed = rows_of(1 - place_ref[1])
            pass_ref[...] = passed.reshape(slots, row_count, order)
            stays = rows_of(place_ref[1])
            stay_ref[:, :, 0:order] = stays.reshape(slots, row_count, order)
            wide = grad.astype(jnp.float32)
            grad_square = jnp.sum(wide * wide, keepdims=True)
            wide = passed.astype(jnp.float32)
            dir_square = jnp.sum(wide * wide, keepdims=True)
            wide = stays.astype(jnp.float32)
            dir_square = dir_square + jnp.sum(wide * wide, keepdims=True)
            row = mask_ref[0:1] * grad_square + mask_ref[1:2] * dir_square
            norm_ref[...] = jnp.broadcast_to(row[None], norm_ref.shape)

        @pl.when(place_ref[0] == 0)
        def _():
            norm_ref[...] = jnp.zeros_like(norm_ref)

    return pl.pallas_call(
        body,
        out_shape=(
            jax.ShapeDtypeStruct((slots, row_count, order + LANES), jnp.bfloat16),
            jax.ShapeDtypeStruct((slots, row_count, order), jnp.bfloat16),
            jax.ShapeDtypeStruct((near_count, 1, LANES), jnp.float32),
        ),
        in_specs=[SMEM, VMEM, VMEM, VMEM, VMEM],
        out_specs=(VMEM, VMEM, VMEM),
        compiler_params=params(12),
        name="precondition",
    )(place, masks, grad_block, left, right)


def fill_slots(place, near_norms, passed, slots):
    slot_count, row_count, width = slots.shape
    order = width - LANES

    def body(place_ref, near_ref, passed_ref, slot_ref, out_ref, rows_ref, sems):
        del slot_ref
        rows_copy = pltpu.make_async_copy(passed_ref, out_ref.at[:, :, 0:order], sems.at[0])

        @pl.when(place_ref[0] == 0)
        def _():
            rows_copy.start()

        total = jnp.sum(near_ref[...], axis=0)
        high = total.astype(jnp.bfloat16).astype(jnp.float32)
        rest = total - high
        middle = rest.astype(jnp.bfloat16).astype(jnp.float32)
        low = rest - middle
        shape = rows_ref.shape[1:]
        row = lax.broadcasted_iota(jnp.int32, shape, 0)
        packed = jnp.where(
            row == 0,
            jnp.broadcast_to(high, shape),
            jnp.where(
                row == 1,
                jnp.broadcast_to(middle, shape),
                jnp.where(row == 2, jnp.broadcast_to(low, shape), 0.0),
            ),
        ).astype(jnp.bfloat16)
        rows_ref[...] = jnp.broadcast_to(packed[None], rows_ref.shape)
        norm_copy = pltpu.make_async_copy(rows_ref, out_ref.at[:, :, order:width], sems.at[1])
        norm_copy.start()
        norm_copy.wait()

        @pl.when(place_ref[0] == 0)
        def _():
            rows_copy.wait()

    return pl.pallas_call(
        body,
        out_shape=jax.ShapeDtypeStruct(slots.shape, slots.dtype),
        in_specs=[SMEM, VMEM, ANY, ANY],
        out_specs=ANY,
        scratch_shapes=[
            pltpu.VMEM((slot_count, row_count, LANES), slots.dtype),
            pltpu.SemaphoreType.DMA((2,)),
        ],
        input_output_aliases={3: 0},
        compiler_params=params(4),
        name="fill_slots",
    )(place, near_norms, passed, slots)


def scale_blocks(owners, slots):
    blocks_here = owners.shape[1]
    slot_count, row_count, width = slots.shape
    order = width - LANES

    def body(owner_ref, slot_ref, out_ref):
        norms = jnp.zeros((row_count, LANES), jnp.float32)
        for p in range(slot_count):
            norms = norms + slot_ref[p, :, order:width].astype(jnp.float32)
        totals = norms[0:1] + (norms[1:2] + norms[2:3])
        columns = jnp.broadcast_to(totals, (LANES, LANES)).T
        ratio = jnp.sqrt(
            columns[:blocks_here] / (columns[blocks_here : 2 * blocks_here] + tiny_term)
        )
        for j in range(blocks_here):
            owner = owner_ref[0, j]
            slot = jnp.where(owner < slot_count, owner, owner - slot_count)
            scale = jnp.broadcast_to(ratio[j : j + 1], (row_count, LANES))
            for c in range(order // LANES):
                at = slice(c * LANES, (c + 1) * LANES)
                rows = slot_ref[slot, :, at].astype(jnp.float32)
                out_ref[j, :, at] = (scale * rows).astype(out_ref.dtype)

    return pl.pallas_call(
        body,
        out_shape=jax.ShapeDtypeStruct((blocks_here, row_count, order), slots.dtype),
        in_specs=[SMEM, VMEM],
        out_specs=VMEM,
        compiler_params=params(4),
        name="scale_blocks",
    )(owners, slots)


def refresh(place, grad_block, left_stats, right_stats):
    order = grad_block.shape[0]
    strip = 64

    def body(place_ref, grad_ref, left_ref, right_ref, left_out, right_out, wide, low, first):
        def one(stat_ref, out_ref, dims):
            grad = grad_ref[...]
            wide[...] = lax.dot_general(grad, grad, dims, preferred_element_type=jnp.float32)

            def shift(i, total):
                at = pl.ds(i * strip, strip)
                on_diagonal = lax.broadcasted_iota(
                    jnp.int32, (strip, order), 1
                ) == i * strip + lax.broadcasted_iota(jnp.int32, (strip, order), 0)
                shifted = stat_decay * stat_ref[at] + wide[at] / order
                shifted = shifted + jnp.where(on_diagonal, ridge_term, 0.0)
                wide[at] = shifted
                return total + jnp.sum(
                    (shifted * shifted).reshape(strip // 8, 8, order), axis=0
                )

            squares = lax.fori_loop(
                0, order // strip, shift, jnp.zeros((8, order), jnp.float32)
            )
            scale = jnp.sqrt(jnp.sum(squares, keepdims=True) + tiny_term)
            start = 1.0 / jnp.sqrt(jnp.sqrt(scale))

            def begin(i, carry):
                at = pl.ds(i * strip, strip)
                on_diagonal = lax.broadcasted_iota(
                    jnp.int32, (strip, order), 1
                ) == i * strip + lax.broadcasted_iota(jnp.int32, (strip, order), 0)
                matrix = wide[at] / scale
                factor = ((jnp.where(on_diagonal, 5.0, 0.0) - matrix) / 4.0).astype(jnp.bfloat16)
                low[0, at] = matrix.astype(jnp.bfloat16)
                low[1, at] = factor
                first[at] = (start * factor.astype(jnp.float32)).astype(jnp.bfloat16)
                return carry

            lax.fori_loop(0, order // strip, begin, 0)

            def dot(a, b):
                return jnp.dot(a, b, preferred_element_type=jnp.float32)

            low[2] = dot(low[1], low[1]).astype(jnp.bfloat16)
            low[1] = dot(low[2], low[2]).astype(jnp.bfloat16)
            wide[...] = dot(low[1], low[0])

            def again(i, carry):
                at = pl.ds(i * strip, strip)
                on_diagonal = lax.broadcasted_iota(
                    jnp.int32, (strip, order), 1
                ) == i * strip + lax.broadcasted_iota(jnp.int32, (strip, order), 0)
                low[2, at] = ((jnp.where(on_diagonal, 5.0, 0.0) - wide[at]) / 4.0).astype(
                    jnp.bfloat16
                )
                return carry

            lax.fori_loop(0, order // strip, again, 0)
            out_ref[...] = dot(first[...], low[2]).astype(jnp.bfloat16)

        @pl.when(place_ref[0] == 1)
        def _():
            one(left_ref, left_out, (((1,), (1,)), ((), ())))
            one(right_ref, right_out, (((0,), (0,)), ((), ())))

        @pl.when(place_ref[0] == 0)
        def _():
            left_out[...] = jnp.zeros_like(left_out)
            right_out[...] = jnp.zeros_like(right_out)

    root = jax.ShapeDtypeStruct((order, order), jnp.bfloat16)
    return pl.pallas_call(
        body,
        out_shape=(root, root),
        in_specs=[SMEM, VMEM, VMEM, VMEM],
        out_specs=(VMEM, VMEM),
        scratch_shapes=[
            pltpu.VMEM((order, order), jnp.float32),
            pltpu.VMEM((3, order, order), jnp.bfloat16),
            pltpu.VMEM((order, order), jnp.bfloat16),
        ],
        compiler_params=params(24),
        name="refresh",
    )(place, grad_block, left_stats, right_stats)


def shards(gradient, owners, left_stats, right_stats, left_roots_old, right_roots_old):
    dp_count = lax.axis_size(DP)
    near_count = lax.axis_size(NEAR)
    my_index = lax.axis_index(DP)
    blocks_here = gradient.shape[1]
    row_count = gradient.shape[2]
    block_width = gradient.shape[3]
    is_mine = owners[0] == my_index
    busy = jnp.any(is_mine).astype(jnp.int32).reshape(1)
    mine = is_mine.astype(jnp.float32)
    masks = jnp.stack(
        [
            jnp.pad(mine, (0, LANES - blocks_here)),
            jnp.pad(mine, (blocks_here, LANES - 2 * blocks_here)),
        ]
    )
    outgoing = place_blocks(owners, gradient[0], dp_count)
    arrived = lax.all_to_all(outgoing, DP, split_axis=0, concat_axis=0, tiled=True)
    grad_block = arrived.reshape(dp_count * row_count, block_width)
    place = jnp.concatenate([busy, lax.axis_index("dp_0h").astype(jnp.int32).reshape(1)])
    stays, passes, norms = precondition(
        place, masks, grad_block, left_roots_old[0, 0], right_roots_old[0, 0], near_count, row_count
    )
    passed = lax.ppermute(passes, "dp_0h", [(0, 1), (1, 0)])
    near_norms = lax.all_to_all(norms, NEAR, split_axis=0, concat_axis=0, tiled=True)
    slots = fill_slots(place, near_norms, passed, stays)
    returned = lax.all_to_all(slots, PAIRS, split_axis=0, concat_axis=0, tiled=True)
    left_root, right_root = refresh(place, grad_block, left_stats[0, 0], right_stats[0, 0])
    update = scale_blocks(owners, returned)[None]
    return (update, left_root[None, None], right_root[None, None])


def solution(mesh):
    finer = Mesh(
        mesh.devices.reshape(2, 2, 8, 2, 4, 2),
        ("dp_0h", "dp_0l", "dp_1", "dp_2", "mp_0", "mp_1"),
    )
    placed = (
        P(MP, None, DP, None),
        P(MP, None),
        P(MP, DP, None, None),
        P(MP, DP, None, None),
        P(MP, DP, None, None),
        P(MP, DP, None, None),
    )
    return jax.shard_map(
        shards,
        mesh=finer,
        in_specs=placed,
        out_specs=(P(MP, None, DP, None), P(MP, DP, None, None), P(MP, DP, None, None)),
        check_vma=False,
    )
```

```python
import jax
import jax.numpy as jnp
from jax import lax
from jax.experimental import pallas as pl
from jax.experimental.pallas import tpu as pltpu
from jax.sharding import Mesh
from jax.sharding import PartitionSpec as P

ITERS = 2
DP = ("dp_0h", "dp_0l", "dp_1", "dp_2")
MP = ("mp_0", "mp_1")
LANES = 128
MIB = 1024 * 1024


stat_decay = 0.9
ridge_term = 0.001
tiny_term = 1e-06

SMEM = pl.BlockSpec(memory_space=pltpu.SMEM)
VMEM = pl.BlockSpec(memory_space=pltpu.VMEM)
ANY = pl.BlockSpec(memory_space=pl.ANY)


def params(mib):
    return pltpu.CompilerParams(vmem_limit_bytes=mib * MIB)


def partner_of(owner, dp_count):
    half = dp_count // 2
    return jnp.where(owner < half, owner + half, owner - half)


def place_blocks(owners, my_index, blocks, dp_count):
    blocks_here, row_count, width = blocks.shape

    def body(owner_ref, index_ref, block_ref, slot_ref, flag_ref):
        busy = jnp.int32(0)
        mine = jnp.int32(0)
        for j in range(blocks_here):
            owner = owner_ref[0, j]
            rows = block_ref[j]
            slot_ref[owner] = rows
            slot_ref[partner_of(owner, dp_count)] = rows
            here = (owner == index_ref[0]).astype(jnp.int32)
            busy = busy + here
            mine = mine + here * j
        flag_ref[0] = busy
        flag_ref[1] = mine

    return pl.pallas_call(
        body,
        out_shape=(
            jax.ShapeDtypeStruct((dp_count, row_count, width), blocks.dtype),
            jax.ShapeDtypeStruct((2,), jnp.int32),
        ),
        in_specs=[SMEM, SMEM, VMEM],
        out_specs=(VMEM, SMEM),
        compiler_params=params(4),
        name="place_blocks",
    )(owners, my_index, blocks)


def precondition(flags, grad_block, left, right, blocks_here, mp_count, row_count):
    order = grad_block.shape[0]
    half = order // 2
    slots = order // row_count

    def body(flag_ref, grad_ref, left_ref, right_ref, stay_ref, pass_ref, norm_ref):
        @pl.when(flag_ref[0] == 1)
        def _():
            grad = grad_ref[...]
            shaded = jnp.dot(grad, right_ref[...], preferred_element_type=jnp.float32)
            direction = jnp.dot(
                left_ref[...], shaded.astype(jnp.bfloat16), preferred_element_type=jnp.float32
            ).astype(jnp.bfloat16)
            pass_ref[...] = direction[:, half:].reshape(slots, row_count, half)
            stay_ref[:, :, 0:half] = direction[:, :half].reshape(slots, row_count, half)
            wide = grad.astype(jnp.float32)
            grad_square = jnp.sum(wide * wide, keepdims=True)
            wide = direction.astype(jnp.float32)
            dir_square = jnp.sum(wide * wide, keepdims=True)
            lane = lax.broadcasted_iota(jnp.int32, (1, LANES), 1)
            row = jnp.where(lane == flag_ref[1], grad_square, 0.0)
            row = row + jnp.where(lane == flag_ref[1] + blocks_here, dir_square, 0.0)
            norm_ref[...] = jnp.broadcast_to(row[None], norm_ref.shape)

        @pl.when(flag_ref[0] == 0)
        def _():
            norm_ref[...] = jnp.zeros_like(norm_ref)

    return pl.pallas_call(
        body,
        out_shape=(
            jax.ShapeDtypeStruct((slots, row_count, half + LANES), jnp.bfloat16),
            jax.ShapeDtypeStruct((slots, row_count, half), jnp.bfloat16),
            jax.ShapeDtypeStruct((mp_count, 1, LANES), jnp.float32),
        ),
        in_specs=[SMEM, VMEM, VMEM, VMEM],
        out_specs=(VMEM, VMEM, VMEM),
        compiler_params=params(12),
        name="precondition",
    )(flags, grad_block, left, right)


def fill_slots(flags, row_norms, passed, slots):
    slot_count, row_count, width = slots.shape
    half = width - LANES

    def body(flag_ref, norm_ref, passed_ref, slot_ref, out_ref, rows_ref, sems):
        del slot_ref
        passed_copy = pltpu.make_async_copy(passed_ref, out_ref.at[:, :, 0:half], sems.at[0])

        @pl.when(flag_ref[0] == 0)
        def _():
            passed_copy.start()

        total = jnp.sum(norm_ref[...], axis=0)
        high = total.astype(jnp.bfloat16).astype(jnp.float32)
        rest = total - high
        middle = rest.astype(jnp.bfloat16).astype(jnp.float32)
        low = rest - middle
        shape = rows_ref.shape[1:]
        row = lax.broadcasted_iota(jnp.int32, shape, 0)
        packed = jnp.where(
            row == 0,
            jnp.broadcast_to(high, shape),
            jnp.where(
                row == 1,
                jnp.broadcast_to(middle, shape),
                jnp.where(row == 2, jnp.broadcast_to(low, shape), 0.0),
            ),
        ).astype(jnp.bfloat16)
        rows_ref[...] = jnp.broadcast_to(packed[None], rows_ref.shape)
        norm_copy = pltpu.make_async_copy(rows_ref, out_ref.at[:, :, half:width], sems.at[1])
        norm_copy.start()
        norm_copy.wait()

        @pl.when(flag_ref[0] == 0)
        def _():
            passed_copy.wait()

    return pl.pallas_call(
        body,
        out_shape=jax.ShapeDtypeStruct(slots.shape, slots.dtype),
        in_specs=[SMEM, VMEM, ANY, ANY],
        out_specs=ANY,
        scratch_shapes=[
            pltpu.VMEM((slot_count, row_count, LANES), slots.dtype),
            pltpu.SemaphoreType.DMA((2,)),
        ],
        input_output_aliases={3: 0},
        compiler_params=params(4),
        name="fill_slots",
    )(flags, row_norms, passed, slots)


def scale_blocks(owners, slots):
    blocks_here = owners.shape[1]
    slot_count, row_count, width = slots.shape
    half = width - LANES

    def body(owner_ref, slot_ref, out_ref):
        norms = jnp.zeros((row_count, LANES), jnp.float32)
        for p in range(slot_count):
            norms = norms + slot_ref[p, :, half:width].astype(jnp.float32)
        totals = norms[0:1] + (norms[1:2] + norms[2:3])
        columns = jnp.broadcast_to(totals, (LANES, LANES)).T
        ratio = jnp.sqrt(
            columns[:blocks_here] / (columns[blocks_here : 2 * blocks_here] + tiny_term)
        )
        for j in range(blocks_here):
            owner = owner_ref[0, j]
            scale = jnp.broadcast_to(ratio[j : j + 1], (row_count, LANES))
            for k, slot in enumerate((owner, partner_of(owner, slot_count))):
                for c in range(0, half, LANES):
                    rows = slot_ref[slot, :, c : c + LANES].astype(jnp.float32)
                    at = slice(k * half + c, k * half + c + LANES)
                    out_ref[j, :, at] = (scale * rows).astype(out_ref.dtype)

    return pl.pallas_call(
        body,
        out_shape=jax.ShapeDtypeStruct((blocks_here, row_count, 2 * half), slots.dtype),
        in_specs=[SMEM, VMEM],
        out_specs=VMEM,
        compiler_params=params(4),
        name="scale_blocks",
    )(owners, slots)


def refresh(flags, grad_block, left_stats, right_stats):
    order = grad_block.shape[0]
    strip = 64

    def body(flag_ref, grad_ref, left_ref, right_ref, left_out, right_out, wide, low, first):
        def one(stat_ref, out_ref, dims):
            grad = grad_ref[...]
            wide[...] = lax.dot_general(grad, grad, dims, preferred_element_type=jnp.float32)

            def shift(i, total):
                at = pl.ds(i * strip, strip)
                on_diagonal = lax.broadcasted_iota(
                    jnp.int32, (strip, order), 1
                ) == i * strip + lax.broadcasted_iota(jnp.int32, (strip, order), 0)
                shifted = stat_decay * stat_ref[at] + wide[at] / order
                shifted = shifted + jnp.where(on_diagonal, ridge_term, 0.0)
                wide[at] = shifted
                return total + jnp.sum(
                    (shifted * shifted).reshape(strip // 8, 8, order), axis=0
                )

            squares = lax.fori_loop(
                0, order // strip, shift, jnp.zeros((8, order), jnp.float32)
            )
            scale = jnp.sqrt(jnp.sum(squares, keepdims=True) + tiny_term)
            start = 1.0 / jnp.sqrt(jnp.sqrt(scale))

            def begin(i, carry):
                at = pl.ds(i * strip, strip)
                on_diagonal = lax.broadcasted_iota(
                    jnp.int32, (strip, order), 1
                ) == i * strip + lax.broadcasted_iota(jnp.int32, (strip, order), 0)
                matrix = wide[at] / scale
                factor = ((jnp.where(on_diagonal, 5.0, 0.0) - matrix) / 4.0).astype(jnp.bfloat16)
                low[0, at] = matrix.astype(jnp.bfloat16)
                low[1, at] = factor
                first[at] = (start * factor.astype(jnp.float32)).astype(jnp.bfloat16)
                return carry

            lax.fori_loop(0, order // strip, begin, 0)

            def dot(a, b):
                return jnp.dot(a, b, preferred_element_type=jnp.float32)

            low[2] = dot(low[1], low[1]).astype(jnp.bfloat16)
            low[1] = dot(low[2], low[2]).astype(jnp.bfloat16)
            wide[...] = dot(low[1], low[0])

            def again(i, carry):
                at = pl.ds(i * strip, strip)
                on_diagonal = lax.broadcasted_iota(
                    jnp.int32, (strip, order), 1
                ) == i * strip + lax.broadcasted_iota(jnp.int32, (strip, order), 0)
                low[2, at] = ((jnp.where(on_diagonal, 5.0, 0.0) - wide[at]) / 4.0).astype(
                    jnp.bfloat16
                )
                return carry

            lax.fori_loop(0, order // strip, again, 0)
            out_ref[...] = dot(first[...], low[2]).astype(jnp.bfloat16)

        @pl.when(flag_ref[0] == 1)
        def _():
            one(left_ref, left_out, (((1,), (1,)), ((), ())))
            one(right_ref, right_out, (((0,), (0,)), ((), ())))

        @pl.when(flag_ref[0] == 0)
        def _():
            left_out[...] = jnp.zeros_like(left_out)
            right_out[...] = jnp.zeros_like(right_out)

    root = jax.ShapeDtypeStruct((order, order), jnp.bfloat16)
    return pl.pallas_call(
        body,
        out_shape=(root, root),
        in_specs=[SMEM, VMEM, VMEM, VMEM],
        out_specs=(VMEM, VMEM),
        scratch_shapes=[
            pltpu.VMEM((order, order), jnp.float32),
            pltpu.VMEM((3, order, order), jnp.bfloat16),
            pltpu.VMEM((order, order), jnp.bfloat16),
        ],
        compiler_params=params(24),
        name="refresh",
    )(flags, grad_block, left_stats, right_stats)


def shards(gradient, owners, left_stats, right_stats, left_roots_old, right_roots_old):
    dp_count = lax.axis_size(DP)
    mp_count = lax.axis_size(MP)
    my_index = lax.axis_index(DP).astype(jnp.int32).reshape(1)
    blocks_here = gradient.shape[1]
    row_count = gradient.shape[2]
    block_width = gradient.shape[3]
    outgoing, flags = place_blocks(owners, my_index, gradient[0], dp_count)
    arrived = lax.all_to_all(outgoing, DP, split_axis=0, concat_axis=0, tiled=True)
    grad_block = arrived.reshape(dp_count * row_count, block_width)
    stays, passes, norms = precondition(
        flags, grad_block, left_roots_old[0, 0], right_roots_old[0, 0], blocks_here, mp_count, row_count
    )
    passed = lax.ppermute(passes, "dp_0h", [(0, 1), (1, 0)])
    row_norms = lax.all_to_all(norms, MP, split_axis=0, concat_axis=0, tiled=True)
    slots = fill_slots(flags, row_norms, passed, stays)
    returned = lax.all_to_all(slots, DP, split_axis=0, concat_axis=0, tiled=True)
    left_root, right_root = refresh(flags, grad_block, left_stats[0, 0], right_stats[0, 0])
    update = scale_blocks(owners, returned)[None]
    return (update, left_root[None, None], right_root[None, None])


def solution(mesh):
    finer = Mesh(
        mesh.devices.reshape(2, 2, 8, 2, 4, 2),
        ("dp_0h", "dp_0l", "dp_1", "dp_2", "mp_0", "mp_1"),
    )
    placed = (
        P(MP, None, DP, None),
        P(MP, None),
        P(MP, DP, None, None),
        P(MP, DP, None, None),
        P(MP, DP, None, None),
        P(MP, DP, None, None),
    )
    return jax.shard_map(
        shards,
        mesh=finer,
        in_specs=placed,
        out_specs=(P(MP, None, DP, None), P(MP, DP, None, None), P(MP, DP, None, None)),
        check_vma=False,
    )
```

```python
import jax
import jax.numpy as jnp
from jax import lax
from jax.experimental import pallas as pl
from jax.experimental.pallas import tpu as pltpu
from jax.sharding import Mesh
from jax.sharding import PartitionSpec as P

ITERS = 2
DP = ("dp_0h", "dp_0l", "dp_1", "dp_2")
MP = ("mp_0", "mp_1")
LANES = 128
TILE = 4
MIB = 1024 * 1024
PLACE_MIB = 54


stat_decay = 0.9
ridge_term = 0.001
tiny_term = 1e-06

SMEM = pl.BlockSpec(memory_space=pltpu.SMEM)
VMEM = pl.BlockSpec(memory_space=pltpu.VMEM)
ANY = pl.BlockSpec(memory_space=pl.ANY)


def params(mib):
    return pltpu.CompilerParams(vmem_limit_bytes=mib * MIB)


def tiles_of(row_count, width):
    return [
        (slice(r, r + TILE), slice(c, c + LANES))
        for c in range(0, width, LANES)
        for r in range(0, row_count, TILE)
    ]


def partner_of(owner, dp_count):
    half = dp_count // 2
    return jnp.where(owner < half, owner + half, owner - half)


def place_blocks(owners, blocks, dp_count):
    blocks_here, row_count, width = blocks.shape

    def body(owner_any, block_any, slot_ref, flag_ref, owner_ref, block_ref, sems):
        fetches = (
            pltpu.make_async_copy(owner_any, owner_ref, sems.at[0]),
            pltpu.make_async_copy(block_any, block_ref, sems.at[1]),
        )
        for fetch in fetches:
            fetch.start()
        for fetch in fetches:
            fetch.wait()
        my_index = lax.axis_index(DP)
        busy = jnp.int32(0)
        mine = jnp.int32(0)
        for j in range(blocks_here):
            owner = owner_ref[0, j]
            rows = block_ref[j]
            slot_ref[owner] = rows
            slot_ref[partner_of(owner, dp_count)] = rows
            here = (owner == my_index).astype(jnp.int32)
            beside = (partner_of(owner, dp_count) == my_index).astype(jnp.int32)
            busy = busy + here
            mine = mine + (here + beside) * j
            flag_ref[2 + j] = owner
        flag_ref[0] = busy
        flag_ref[1] = mine

    return pl.pallas_call(
        body,
        out_shape=(
            pltpu.VMEM((dp_count, row_count, width), blocks.dtype),
            pltpu.SMEM((2 + blocks_here,), jnp.int32),
        ),
        in_specs=[ANY, ANY],
        out_specs=(VMEM, SMEM),
        scratch_shapes=[
            pltpu.SMEM(owners.shape, owners.dtype),
            pltpu.VMEM(blocks.shape, blocks.dtype),
            pltpu.SemaphoreType.DMA((2,)),
        ],
        compiler_params=params(PLACE_MIB),
        name="place_blocks",
    )(owners, blocks)


def precondition(flags, grad_block, left, right, blocks_here, mp_count, row_count):
    order = grad_block.shape[0]
    half = order // 2
    slots = order // row_count
    strip = 128

    def body(flag_ref, grad_ref, left_ref, right_ref, stay_ref, pass_ref, norm_ref):
        def squares_of(total, rows):
            wide = rows.astype(jnp.float32)
            return total + jnp.sum((wide * wide).reshape(strip // 8, 8, order), axis=0)

        def write_norm(lane_of, total):
            lane = lax.broadcasted_iota(jnp.int32, (1, LANES), 1)
            row = jnp.where(lane == lane_of, jnp.sum(total, keepdims=True), 0.0)
            norm_ref[...] = jnp.broadcast_to(row[None], norm_ref.shape)

        @pl.when(flag_ref[0] == 1)
        def _():
            shaded = jnp.dot(grad_ref[...], right_ref[...], preferred_element_type=jnp.float32)
            shaded = shaded.astype(jnp.bfloat16)
            total = jnp.zeros((8, order), jnp.float32)
            for i in range(order // strip):
                rows = jnp.dot(
                    left_ref[i * strip : (i + 1) * strip], shaded, preferred_element_type=jnp.float32
                ).astype(jnp.bfloat16)
                at = slice(i * strip // row_count, (i + 1) * strip // row_count)
                stay_ref[at] = rows[:, :half].reshape(strip // row_count, row_count, half)
                pass_ref[at] = rows[:, half:].reshape(strip // row_count, row_count, half)
                total = squares_of(total, rows)
            write_norm(flag_ref[1] + blocks_here, total)

        @pl.when(flag_ref[0] == 0)
        def _():
            total = jnp.zeros((8, order), jnp.float32)
            for i in range(order // strip):
                total = squares_of(total, grad_ref[i * strip : (i + 1) * strip])
            write_norm(flag_ref[1], total)

    return pl.pallas_call(
        body,
        out_shape=(
            pltpu.VMEM((slots, row_count, half), jnp.bfloat16),
            pltpu.VMEM((slots, row_count, half), jnp.bfloat16),
            pltpu.VMEM((mp_count, 1, LANES), jnp.float32),
        ),
        in_specs=[SMEM, VMEM, VMEM, VMEM],
        out_specs=(VMEM, VMEM, VMEM),
        compiler_params=params(12),
        name="precondition",
    )(flags, grad_block, left, right)


def fill_slots(flags, row_norms, passed, stays):
    slot_count, row_count, half = stays.shape
    tiles = row_count * half // (TILE * LANES)

    def body(flag_ref, norm_ref, passed_ref, stay_ref, out_ref):
        total = jnp.sum(norm_ref[...], axis=0)
        high = total.astype(jnp.bfloat16).astype(jnp.float32)
        rest = total - high
        middle = rest.astype(jnp.bfloat16).astype(jnp.float32)
        low = rest - middle
        shape = (TILE, LANES)
        row = lax.broadcasted_iota(jnp.int32, shape, 0)
        packed = jnp.where(
            row == 0,
            jnp.broadcast_to(high, shape),
            jnp.where(
                row == 1,
                jnp.broadcast_to(middle, shape),
                jnp.where(row == 2, jnp.broadcast_to(low, shape), 0.0),
            ),
        ).astype(jnp.bfloat16)
        out_ref[:, tiles] = jnp.broadcast_to(packed[None], (slot_count, TILE, LANES))

        def fill(rows_ref):
            for t, (rows, lanes) in enumerate(tiles_of(row_count, half)):
                out_ref[:, t] = rows_ref[:, rows, lanes]

        @pl.when(flag_ref[0] == 1)
        def _():
            fill(stay_ref)

        @pl.when(flag_ref[0] == 0)
        def _():
            fill(passed_ref)

    return pl.pallas_call(
        body,
        out_shape=jax.ShapeDtypeStruct((slot_count, tiles + 1, TILE, LANES), stays.dtype),
        in_specs=[SMEM, VMEM, VMEM, VMEM],
        out_specs=VMEM,
        compiler_params=params(4),
        name="fill_slots",
    )(flags, row_norms, passed, stays)


def scale_blocks(flags, slots, row_count):
    blocks_here = flags.shape[0] - 2
    slot_count = slots.shape[0]
    tiles = slots.shape[1] - 1
    half = tiles * TILE * LANES // row_count

    def body(flag_ref, slot_ref, out_ref):
        norms = jnp.sum(slot_ref[:, tiles].astype(jnp.float32), axis=0)
        totals = norms[0:1] + (norms[1:2] + norms[2:3])
        columns = jnp.broadcast_to(totals, (LANES, LANES)).T
        ratio = jnp.sqrt(
            columns[:blocks_here] / (columns[blocks_here : 2 * blocks_here] + tiny_term)
        )
        for j in range(blocks_here):
            owner = flag_ref[2 + j]
            scale = jnp.broadcast_to(ratio[j : j + 1], (TILE, LANES))
            for k, slot in enumerate((owner, partner_of(owner, slot_count))):
                for t, (rows, lanes) in enumerate(tiles_of(row_count, half)):
                    at = slice(k * half + lanes.start, k * half + lanes.stop)
                    tile = slot_ref[slot, t].astype(jnp.float32)
                    out_ref[j, rows, at] = (scale * tile).astype(out_ref.dtype)

    return pl.pallas_call(
        body,
        out_shape=jax.ShapeDtypeStruct((blocks_here, row_count, 2 * half), slots.dtype),
        in_specs=[SMEM, VMEM],
        out_specs=VMEM,
        compiler_params=params(4),
        name="scale_blocks",
    )(flags, slots)


def refresh(flags, grad_block, left_stats, right_stats):
    order = grad_block.shape[0]
    strip = 64

    def body(flag_ref, grad_ref, left_ref, right_ref, left_out, right_out, wide, low, first):
        def one(stat_ref, out_ref, dims):
            grad = grad_ref[...]
            wide[...] = lax.dot_general(grad, grad, dims, preferred_element_type=jnp.float32)

            def shift(i, total):
                at = pl.ds(i * strip, strip)
                on_diagonal = lax.broadcasted_iota(
                    jnp.int32, (strip, order), 1
                ) == i * strip + lax.broadcasted_iota(jnp.int32, (strip, order), 0)
                shifted = stat_decay * stat_ref[at] + wide[at] / order
                shifted = shifted + jnp.where(on_diagonal, ridge_term, 0.0)
                wide[at] = shifted
                return total + jnp.sum(
                    (shifted * shifted).reshape(strip // 8, 8, order), axis=0
                )

            squares = lax.fori_loop(
                0, order // strip, shift, jnp.zeros((8, order), jnp.float32)
            )
            scale = jnp.sqrt(jnp.sum(squares, keepdims=True) + tiny_term)
            start = 1.0 / jnp.sqrt(jnp.sqrt(scale))

            def begin(i, carry):
                at = pl.ds(i * strip, strip)
                on_diagonal = lax.broadcasted_iota(
                    jnp.int32, (strip, order), 1
                ) == i * strip + lax.broadcasted_iota(jnp.int32, (strip, order), 0)
                matrix = wide[at] / scale
                factor = ((jnp.where(on_diagonal, 5.0, 0.0) - matrix) / 4.0).astype(jnp.bfloat16)
                low[0, at] = matrix.astype(jnp.bfloat16)
                low[1, at] = factor
                first[at] = (start * factor.astype(jnp.float32)).astype(jnp.bfloat16)
                return carry

            lax.fori_loop(0, order // strip, begin, 0)

            def dot(a, b):
                return jnp.dot(a, b, preferred_element_type=jnp.float32)

            low[2] = dot(low[1], low[1]).astype(jnp.bfloat16)
            low[1] = dot(low[2], low[2]).astype(jnp.bfloat16)
            wide[...] = dot(low[1], low[0])

            def again(i, carry):
                at = pl.ds(i * strip, strip)
                on_diagonal = lax.broadcasted_iota(
                    jnp.int32, (strip, order), 1
                ) == i * strip + lax.broadcasted_iota(jnp.int32, (strip, order), 0)
                low[2, at] = ((jnp.where(on_diagonal, 5.0, 0.0) - wide[at]) / 4.0).astype(
                    jnp.bfloat16
                )
                return carry

            lax.fori_loop(0, order // strip, again, 0)
            out_ref[...] = dot(first[...], low[2]).astype(jnp.bfloat16)

        @pl.when(flag_ref[0] == 1)
        def _():
            one(left_ref, left_out, (((1,), (1,)), ((), ())))
            one(right_ref, right_out, (((0,), (0,)), ((), ())))

        @pl.when(flag_ref[0] == 0)
        def _():
            left_out[...] = jnp.zeros_like(left_out)
            right_out[...] = jnp.zeros_like(right_out)

    root = jax.ShapeDtypeStruct((order, order), jnp.bfloat16)
    return pl.pallas_call(
        body,
        out_shape=(root, root),
        in_specs=[SMEM, VMEM, VMEM, VMEM],
        out_specs=(VMEM, VMEM),
        scratch_shapes=[
            pltpu.VMEM((order, order), jnp.float32),
            pltpu.VMEM((3, order, order), jnp.bfloat16),
            pltpu.VMEM((order, order), jnp.bfloat16),
        ],
        compiler_params=params(24),
        name="refresh",
    )(flags, grad_block, left_stats, right_stats)


def shards(gradient, owners, left_stats, right_stats, left_roots_old, right_roots_old):
    dp_count = lax.axis_size(DP)
    mp_count = lax.axis_size(MP)
    blocks_here = gradient.shape[1]
    row_count = gradient.shape[2]
    block_width = gradient.shape[3]
    outgoing, flags = place_blocks(owners, gradient[0], dp_count)
    arrived = lax.all_to_all(outgoing, DP, split_axis=0, concat_axis=0, tiled=True)
    grad_block = arrived.reshape(dp_count * row_count, block_width)
    stays, passes, norms = precondition(
        flags, grad_block, left_roots_old[0, 0], right_roots_old[0, 0], blocks_here, mp_count, row_count
    )
    passed = lax.ppermute(passes, "dp_0h", [(0, 1), (1, 0)])
    row_norms = lax.all_to_all(norms, MP, split_axis=0, concat_axis=0, tiled=True)
    slots = fill_slots(flags, row_norms, passed, stays)
    returned = lax.all_to_all(slots, DP, split_axis=0, concat_axis=0, tiled=True)
    left_root, right_root = refresh(flags, grad_block, left_stats[0, 0], right_stats[0, 0])
    update = scale_blocks(flags, returned, row_count)[None]
    return (update, left_root[None, None], right_root[None, None])


def solution(mesh):
    finer = Mesh(
        mesh.devices.reshape(2, 2, 8, 2, 4, 2),
        ("dp_0h", "dp_0l", "dp_1", "dp_2", "mp_0", "mp_1"),
    )
    placed = (
        P(MP, None, DP, None),
        P(MP, None),
        P(MP, DP, None, None),
        P(MP, DP, None, None),
        P(MP, DP, None, None),
        P(MP, DP, None, None),
    )
    return jax.shard_map(
        shards,
        mesh=finer,
        in_specs=placed,
        out_specs=(P(MP, None, DP, None), P(MP, DP, None, None), P(MP, DP, None, None)),
        check_vma=False,
    )
```

```python
import jax
import jax.numpy as jnp
from jax import lax
from jax.experimental import pallas as pl
from jax.experimental.pallas import tpu as pltpu
from jax.sharding import Mesh
from jax.sharding import PartitionSpec as P

ITERS = 2
DP = ("dp_0h", "dp_0l", "dp_1", "dp_2")
MP = ("mp_0", "mp_1")
LANES = 128
TILE = 4
PIECES = 4
MIB = 1024 * 1024
PLACE_MIB = 54


stat_decay = 0.9
ridge_term = 0.001
tiny_term = 1e-06

SMEM = pl.BlockSpec(memory_space=pltpu.SMEM)
VMEM = pl.BlockSpec(memory_space=pltpu.VMEM)
ANY = pl.BlockSpec(memory_space=pl.ANY)


def params(mib):
    return pltpu.CompilerParams(vmem_limit_bytes=mib * MIB)


def tiles_of(row_count, width):
    return [
        (slice(r, r + TILE), slice(c, c + LANES))
        for c in range(0, width, LANES)
        for r in range(0, row_count, TILE)
    ]


def partner_of(owner, dp_count):
    half = dp_count // 2
    return jnp.where(owner < half, owner + half, owner - half)


def place_blocks(owners, blocks, dp_count):
    blocks_here, row_count, width = blocks.shape
    per_piece = blocks_here // PIECES

    def body(owner_any, block_any, slot_ref, flag_ref, owner_ref, block_ref, sems):
        owner_fetch = pltpu.make_async_copy(owner_any, owner_ref, sems.at[PIECES])
        owner_fetch.start()
        fetches = []
        for piece in range(PIECES):
            at = pl.ds(piece * per_piece, per_piece)
            fetch = pltpu.make_async_copy(block_any.at[at], block_ref.at[at], sems.at[piece])
            fetch.start()
            fetches.append(fetch)
        owner_fetch.wait()
        my_index = lax.axis_index(DP)
        busy = jnp.int32(0)
        mine = jnp.int32(0)
        for j in range(blocks_here):
            if j % per_piece == 0:
                fetches[j // per_piece].wait()
            owner = owner_ref[0, j]
            rows = block_ref[j]
            slot_ref[owner] = rows
            slot_ref[partner_of(owner, dp_count)] = rows
            here = (owner == my_index).astype(jnp.int32)
            beside = (partner_of(owner, dp_count) == my_index).astype(jnp.int32)
            busy = busy + here
            mine = mine + (here + beside) * j
            flag_ref[2 + j] = owner
        flag_ref[0] = busy
        flag_ref[1] = mine

    return pl.pallas_call(
        body,
        out_shape=(
            pltpu.VMEM((dp_count, row_count, width), blocks.dtype),
            pltpu.SMEM((2 + blocks_here,), jnp.int32),
        ),
        in_specs=[ANY, ANY],
        out_specs=(VMEM, SMEM),
        scratch_shapes=[
            pltpu.SMEM(owners.shape, owners.dtype),
            pltpu.VMEM(blocks.shape, blocks.dtype),
            pltpu.SemaphoreType.DMA((PIECES + 1,)),
        ],
        compiler_params=params(PLACE_MIB),
        name="place_blocks",
    )(owners, blocks)


def precondition(flags, grad_block, left, right, blocks_here, mp_count, row_count):
    order = grad_block.shape[0]
    half = order // 2
    slots = order // row_count
    strip = 128

    def body(flag_ref, grad_ref, left_ref, right_ref, stay_ref, pass_ref, norm_ref):
        def squares_of(total, rows):
            wide = rows.astype(jnp.float32)
            return total + jnp.sum((wide * wide).reshape(strip // 8, 8, order), axis=0)

        def write_norm(lane_of, total):
            lane = lax.broadcasted_iota(jnp.int32, (1, LANES), 1)
            row = jnp.where(lane == lane_of, jnp.sum(total, keepdims=True), 0.0)
            norm_ref[...] = jnp.broadcast_to(row[None], norm_ref.shape)

        @pl.when(flag_ref[0] == 1)
        def _():
            shaded = jnp.dot(grad_ref[...], right_ref[...], preferred_element_type=jnp.float32)
            shaded = shaded.astype(jnp.bfloat16)
            total = jnp.zeros((8, order), jnp.float32)
            for i in range(order // strip):
                rows = jnp.dot(
                    left_ref[i * strip : (i + 1) * strip], shaded, preferred_element_type=jnp.float32
                ).astype(jnp.bfloat16)
                at = slice(i * strip // row_count, (i + 1) * strip // row_count)
                stay_ref[at] = rows[:, :half].reshape(strip // row_count, row_count, half)
                pass_ref[at] = rows[:, half:].reshape(strip // row_count, row_count, half)
                total = squares_of(total, rows)
            write_norm(flag_ref[1] + blocks_here, total)

        @pl.when(flag_ref[0] == 0)
        def _():
            total = jnp.zeros((8, order), jnp.float32)
            for i in range(order // strip):
                total = squares_of(total, grad_ref[i * strip : (i + 1) * strip])
            write_norm(flag_ref[1], total)

    return pl.pallas_call(
        body,
        out_shape=(
            pltpu.VMEM((slots, row_count, half), jnp.bfloat16),
            pltpu.VMEM((slots, row_count, half), jnp.bfloat16),
            pltpu.VMEM((mp_count, 1, LANES), jnp.float32),
        ),
        in_specs=[SMEM, VMEM, VMEM, VMEM],
        out_specs=(VMEM, VMEM, VMEM),
        compiler_params=params(12),
        name="precondition",
    )(flags, grad_block, left, right)


def fill_slots(flags, row_norms, passed, stays):
    slot_count, row_count, half = stays.shape
    tiles = row_count * half // (TILE * LANES)
    per_piece = slot_count // PIECES

    def body(flag_ref, norm_ref, passed_ref, stay_ref, out_any, out_ref, sems):
        total = jnp.sum(norm_ref[...], axis=0)
        high = total.astype(jnp.bfloat16).astype(jnp.float32)
        rest = total - high
        middle = rest.astype(jnp.bfloat16).astype(jnp.float32)
        low = rest - middle
        shape = (TILE, LANES)
        row = lax.broadcasted_iota(jnp.int32, shape, 0)
        packed = jnp.where(
            row == 0,
            jnp.broadcast_to(high, shape),
            jnp.where(
                row == 1,
                jnp.broadcast_to(middle, shape),
                jnp.where(row == 2, jnp.broadcast_to(low, shape), 0.0),
            ),
        ).astype(jnp.bfloat16)

        def fill(rows_ref):
            copies = []
            for piece in range(PIECES):
                at = pl.ds(piece * per_piece, per_piece)
                out_ref[at, tiles] = jnp.broadcast_to(packed[None], (per_piece, TILE, LANES))
                for t, (rows, lanes) in enumerate(tiles_of(row_count, half)):
                    out_ref[at, t] = rows_ref[at, rows, lanes]
                copy = pltpu.make_async_copy(out_ref.at[at], out_any.at[at], sems.at[piece])
                copy.start()
                copies.append(copy)
            for copy in copies:
                copy.wait()

        @pl.when(flag_ref[0] == 1)
        def _():
            fill(stay_ref)

        @pl.when(flag_ref[0] == 0)
        def _():
            fill(passed_ref)

    return pl.pallas_call(
        body,
        out_shape=jax.ShapeDtypeStruct((slot_count, tiles + 1, TILE, LANES), stays.dtype),
        in_specs=[SMEM, VMEM, VMEM, VMEM],
        out_specs=ANY,
        scratch_shapes=[
            pltpu.VMEM((slot_count, tiles + 1, TILE, LANES), stays.dtype),
            pltpu.SemaphoreType.DMA((PIECES,)),
        ],
        compiler_params=params(4),
        name="fill_slots",
    )(flags, row_norms, passed, stays)


def scale_blocks(flags, slots, row_count):
    blocks_here = flags.shape[0] - 2
    slot_count = slots.shape[0]
    tiles = slots.shape[1] - 1
    half = tiles * TILE * LANES // row_count
    per_piece = blocks_here // PIECES

    def body(flag_ref, slot_ref, out_any, out_ref, sems):
        copies = []
        norms = jnp.sum(slot_ref[:, tiles].astype(jnp.float32), axis=0)
        totals = norms[0:1] + (norms[1:2] + norms[2:3])
        columns = jnp.broadcast_to(totals, (LANES, LANES)).T
        ratio = jnp.sqrt(
            columns[:blocks_here] / (columns[blocks_here : 2 * blocks_here] + tiny_term)
        )
        for j in range(blocks_here):
            owner = flag_ref[2 + j]
            scale = jnp.broadcast_to(ratio[j : j + 1], (TILE, LANES))
            for k, slot in enumerate((owner, partner_of(owner, slot_count))):
                for t, (rows, lanes) in enumerate(tiles_of(row_count, half)):
                    at = slice(k * half + lanes.start, k * half + lanes.stop)
                    tile = slot_ref[slot, t].astype(jnp.float32)
                    out_ref[j, rows, at] = (scale * tile).astype(out_ref.dtype)
            if (j + 1) % per_piece == 0:
                piece = j // per_piece
                at = pl.ds(piece * per_piece, per_piece)
                copy = pltpu.make_async_copy(out_ref.at[at], out_any.at[at], sems.at[piece])
                copy.start()
                copies.append(copy)
        for copy in copies:
            copy.wait()

    return pl.pallas_call(
        body,
        out_shape=jax.ShapeDtypeStruct((blocks_here, row_count, 2 * half), slots.dtype),
        in_specs=[SMEM, VMEM],
        out_specs=ANY,
        scratch_shapes=[
            pltpu.VMEM((blocks_here, row_count, 2 * half), slots.dtype),
            pltpu.SemaphoreType.DMA((PIECES,)),
        ],
        compiler_params=params(4),
        name="scale_blocks",
    )(flags, slots)


def refresh(flags, grad_block, left_stats, right_stats):
    order = grad_block.shape[0]
    strip = 64

    def body(flag_ref, grad_ref, left_ref, right_ref, left_out, right_out, wide, low, first):
        def one(stat_ref, out_ref, dims):
            grad = grad_ref[...]
            wide[...] = lax.dot_general(grad, grad, dims, preferred_element_type=jnp.float32)

            def shift(i, total):
                at = pl.ds(i * strip, strip)
                on_diagonal = lax.broadcasted_iota(
                    jnp.int32, (strip, order), 1
                ) == i * strip + lax.broadcasted_iota(jnp.int32, (strip, order), 0)
                shifted = stat_decay * stat_ref[at] + wide[at] / order
                shifted = shifted + jnp.where(on_diagonal, ridge_term, 0.0)
                wide[at] = shifted
                return total + jnp.sum(
                    (shifted * shifted).reshape(strip // 8, 8, order), axis=0
                )

            squares = lax.fori_loop(
                0, order // strip, shift, jnp.zeros((8, order), jnp.float32)
            )
            scale = jnp.sqrt(jnp.sum(squares, keepdims=True) + tiny_term)
            start = 1.0 / jnp.sqrt(jnp.sqrt(scale))

            def begin(i, carry):
                at = pl.ds(i * strip, strip)
                on_diagonal = lax.broadcasted_iota(
                    jnp.int32, (strip, order), 1
                ) == i * strip + lax.broadcasted_iota(jnp.int32, (strip, order), 0)
                matrix = wide[at] / scale
                factor = ((jnp.where(on_diagonal, 5.0, 0.0) - matrix) / 4.0).astype(jnp.bfloat16)
                low[0, at] = matrix.astype(jnp.bfloat16)
                low[1, at] = factor
                first[at] = (start * factor.astype(jnp.float32)).astype(jnp.bfloat16)
                return carry

            lax.fori_loop(0, order // strip, begin, 0)

            def dot(a, b):
                return jnp.dot(a, b, preferred_element_type=jnp.float32)

            low[2] = dot(low[1], low[1]).astype(jnp.bfloat16)
            low[1] = dot(low[2], low[2]).astype(jnp.bfloat16)
            wide[...] = dot(low[1], low[0])

            def again(i, carry):
                at = pl.ds(i * strip, strip)
                on_diagonal = lax.broadcasted_iota(
                    jnp.int32, (strip, order), 1
                ) == i * strip + lax.broadcasted_iota(jnp.int32, (strip, order), 0)
                low[2, at] = ((jnp.where(on_diagonal, 5.0, 0.0) - wide[at]) / 4.0).astype(
                    jnp.bfloat16
                )
                return carry

            lax.fori_loop(0, order // strip, again, 0)
            out_ref[...] = dot(first[...], low[2]).astype(jnp.bfloat16)

        @pl.when(flag_ref[0] == 1)
        def _():
            one(left_ref, left_out, (((1,), (1,)), ((), ())))
            one(right_ref, right_out, (((0,), (0,)), ((), ())))

        @pl.when(flag_ref[0] == 0)
        def _():
            left_out[...] = jnp.zeros_like(left_out)
            right_out[...] = jnp.zeros_like(right_out)

    root = jax.ShapeDtypeStruct((order, order), jnp.bfloat16)
    return pl.pallas_call(
        body,
        out_shape=(root, root),
        in_specs=[SMEM, VMEM, VMEM, VMEM],
        out_specs=(VMEM, VMEM),
        scratch_shapes=[
            pltpu.VMEM((order, order), jnp.float32),
            pltpu.VMEM((3, order, order), jnp.bfloat16),
            pltpu.VMEM((order, order), jnp.bfloat16),
        ],
        compiler_params=params(24),
        name="refresh",
    )(flags, grad_block, left_stats, right_stats)


def shards(gradient, owners, left_stats, right_stats, left_roots_old, right_roots_old):
    dp_count = lax.axis_size(DP)
    mp_count = lax.axis_size(MP)
    blocks_here = gradient.shape[1]
    row_count = gradient.shape[2]
    block_width = gradient.shape[3]
    outgoing, flags = place_blocks(owners, gradient[0], dp_count)
    arrived = lax.all_to_all(outgoing, DP, split_axis=0, concat_axis=0, tiled=True)
    grad_block = arrived.reshape(dp_count * row_count, block_width)
    stays, passes, norms = precondition(
        flags, grad_block, left_roots_old[0, 0], right_roots_old[0, 0], blocks_here, mp_count, row_count
    )
    passed = lax.ppermute(passes, "dp_0h", [(0, 1), (1, 0)])
    row_norms = lax.all_to_all(norms, MP, split_axis=0, concat_axis=0, tiled=True)
    slots = fill_slots(flags, row_norms, passed, stays)
    returned = lax.all_to_all(slots, DP, split_axis=0, concat_axis=0, tiled=True)
    left_root, right_root = refresh(flags, grad_block, left_stats[0, 0], right_stats[0, 0])
    update = scale_blocks(flags, returned, row_count)[None]
    return (update, left_root[None, None], right_root[None, None])


def solution(mesh):
    finer = Mesh(
        mesh.devices.reshape(2, 2, 8, 2, 4, 2),
        ("dp_0h", "dp_0l", "dp_1", "dp_2", "mp_0", "mp_1"),
    )
    placed = (
        P(MP, None, DP, None),
        P(MP, None),
        P(MP, DP, None, None),
        P(MP, DP, None, None),
        P(MP, DP, None, None),
        P(MP, DP, None, None),
    )
    return jax.shard_map(
        shards,
        mesh=finer,
        in_specs=placed,
        out_specs=(P(MP, None, DP, None), P(MP, DP, None, None), P(MP, DP, None, None)),
        check_vma=False,
    )
```

```python
import jax
import jax.numpy as jnp
from jax import lax
from jax.experimental import pallas as pl
from jax.experimental.pallas import tpu as pltpu
from jax.sharding import Mesh
from jax.sharding import PartitionSpec as P

ITERS = 2
DP = ("dp_0h", "dp_0l", "dp_1", "dp_2")
MP = ("mp_0", "mp_1")
LANES = 128
TILE = 4
PIECES = 4
MIB = 1024 * 1024
PLACE_MIB = 54


stat_decay = 0.9
ridge_term = 0.001
tiny_term = 1e-06

SMEM = pl.BlockSpec(memory_space=pltpu.SMEM)
VMEM = pl.BlockSpec(memory_space=pltpu.VMEM)
ANY = pl.BlockSpec(memory_space=pl.ANY)


def params(mib):
    return pltpu.CompilerParams(vmem_limit_bytes=mib * MIB)


def tiles_of(row_count, width):
    return [
        (slice(r, r + TILE), slice(c, c + LANES))
        for c in range(0, width, LANES)
        for r in range(0, row_count, TILE)
    ]


def partner_of(owner, dp_count):
    half = dp_count // 2
    return jnp.where(owner < half, owner + half, owner - half)


def place_blocks(owners, blocks, dp_count):
    blocks_here, row_count, width = blocks.shape
    per_piece = blocks_here // PIECES

    def body(owner_any, block_any, slot_ref, flag_ref, owner_ref, block_ref, sems):
        owner_fetch = pltpu.make_async_copy(owner_any, owner_ref, sems.at[PIECES])
        owner_fetch.start()
        fetches = []
        for piece in range(PIECES):
            at = pl.ds(piece * per_piece, per_piece)
            fetch = pltpu.make_async_copy(block_any.at[at], block_ref.at[at], sems.at[piece])
            fetch.start()
            fetches.append(fetch)
        owner_fetch.wait()
        my_index = lax.axis_index(DP)
        busy = jnp.int32(0)
        mine = jnp.int32(0)
        for j in range(blocks_here):
            if j % per_piece == 0:
                fetches[j // per_piece].wait()
            owner = owner_ref[0, j]
            rows = block_ref[j]
            slot_ref[owner] = rows
            slot_ref[partner_of(owner, dp_count)] = rows
            here = (owner == my_index).astype(jnp.int32)
            beside = (partner_of(owner, dp_count) == my_index).astype(jnp.int32)
            busy = busy + here
            mine = mine + (here + beside) * j
            flag_ref[2 + j] = owner
        flag_ref[0] = busy
        flag_ref[1] = mine

    return pl.pallas_call(
        body,
        out_shape=(
            pltpu.VMEM((dp_count, row_count, width), blocks.dtype),
            pltpu.SMEM((2 + blocks_here,), jnp.int32),
        ),
        in_specs=[ANY, ANY],
        out_specs=(VMEM, SMEM),
        scratch_shapes=[
            pltpu.SMEM(owners.shape, owners.dtype),
            pltpu.VMEM(blocks.shape, blocks.dtype),
            pltpu.SemaphoreType.DMA((PIECES + 1,)),
        ],
        compiler_params=params(PLACE_MIB),
        name="place_blocks",
    )(owners, blocks)


def precondition(flags, grad_block, left, right, blocks_here, row_count):
    order = grad_block.shape[0]
    slots = order // row_count
    tiles = row_count * order // (TILE * LANES)
    strip = order // PIECES
    per_piece = slots // PIECES

    def body(flag_ref, grad_ref, left_ref, right_ref, out_any, out_ref, sems):
        def squares_of(total, rows):
            wide = rows.astype(jnp.float32)
            return total + jnp.sum((wide * wide).reshape(strip // 8, 8, order), axis=0)

        def send_norm(lane_of, total):
            square = jnp.sum(total, keepdims=True)
            high = square.astype(jnp.bfloat16).astype(jnp.float32)
            rest = square - high
            middle = rest.astype(jnp.bfloat16).astype(jnp.float32)
            low = rest - middle
            lane = lax.broadcasted_iota(jnp.int32, (TILE, LANES), 1)
            row = lax.broadcasted_iota(jnp.int32, (TILE, LANES), 0)
            part = jnp.where(row == 0, high, jnp.where(row == 1, middle, low))
            packed = jnp.where((lane == lane_of) & (row < 3), part, 0.0).astype(jnp.bfloat16)
            out_ref[:, tiles] = jnp.broadcast_to(packed[None], (slots, TILE, LANES))
            copy = pltpu.make_async_copy(out_ref.at[:, tiles], out_any.at[:, tiles], sems.at[PIECES])
            copy.start()
            return copy

        @pl.when(flag_ref[0] == 1)
        def _():
            shaded = jnp.dot(grad_ref[...], right_ref[...], preferred_element_type=jnp.float32)
            shaded = shaded.astype(jnp.bfloat16)
            total = jnp.zeros((8, order), jnp.float32)
            copies = []
            for i in range(PIECES):
                rows = jnp.dot(
                    left_ref[i * strip : (i + 1) * strip], shaded, preferred_element_type=jnp.float32
                ).astype(jnp.bfloat16)
                at = pl.ds(i * per_piece, per_piece)
                by_slot = rows.reshape(per_piece, row_count, order)
                for t, (part, lanes) in enumerate(tiles_of(row_count, order)):
                    out_ref[at, t] = by_slot[:, part, lanes]
                copy = pltpu.make_async_copy(
                    out_ref.at[at, pl.ds(0, tiles)], out_any.at[at, pl.ds(0, tiles)], sems.at[i]
                )
                copy.start()
                copies.append(copy)
                total = squares_of(total, rows)
            copies.append(send_norm(flag_ref[1] + blocks_here, total))
            for copy in copies:
                copy.wait()

        @pl.when(flag_ref[0] == 0)
        def _():
            total = jnp.zeros((8, order), jnp.float32)
            for i in range(PIECES):
                total = squares_of(total, grad_ref[i * strip : (i + 1) * strip])
            send_norm(flag_ref[1], total).wait()

    shape = (slots, tiles + 1, TILE, LANES)
    return pl.pallas_call(
        body,
        out_shape=jax.ShapeDtypeStruct(shape, jnp.bfloat16),
        in_specs=[SMEM, VMEM, VMEM, VMEM],
        out_specs=ANY,
        scratch_shapes=[
            pltpu.VMEM(shape, jnp.bfloat16),
            pltpu.SemaphoreType.DMA((PIECES + 1,)),
        ],
        compiler_params=params(12),
        name="precondition",
    )(flags, grad_block, left, right)


def add_norms(slots, done, mp_count):
    tiles = slots.shape[1] - 1

    def body(slot_ref, done_ref, norm_ref):
        del done_ref
        parts = jnp.sum(slot_ref[:, tiles].astype(jnp.float32), axis=0)
        norms = parts[0:1] + (parts[1:2] + parts[2:3])
        norm_ref[...] = jnp.broadcast_to(norms[None], norm_ref.shape)

    return pl.pallas_call(
        body,
        out_shape=pltpu.VMEM((mp_count, 1, LANES), jnp.float32),
        in_specs=[VMEM, SMEM],
        out_specs=VMEM,
        compiler_params=params(4),
        name="add_norms",
    )(slots, done)


def scale_blocks(flags, row_norms, slots, row_count):
    blocks_here = flags.shape[0] - 2
    tiles = slots.shape[1] - 1
    order = tiles * TILE * LANES // row_count
    per_piece = blocks_here // PIECES

    def body(flag_ref, norm_ref, slot_ref, out_any, out_ref, sems):
        copies = []
        totals = jnp.sum(norm_ref[...], axis=0)
        columns = jnp.broadcast_to(totals, (LANES, LANES)).T
        ratio = jnp.sqrt(
            columns[:blocks_here] / (columns[blocks_here : 2 * blocks_here] + tiny_term)
        )
        for j in range(blocks_here):
            owner = flag_ref[2 + j]
            scale = jnp.broadcast_to(ratio[j : j + 1], (TILE, LANES))
            for t, (rows, lanes) in enumerate(tiles_of(row_count, order)):
                tile = slot_ref[owner, t].astype(jnp.float32)
                out_ref[j, rows, lanes] = (scale * tile).astype(out_ref.dtype)
            if (j + 1) % per_piece == 0:
                piece = j // per_piece
                at = pl.ds(piece * per_piece, per_piece)
                copy = pltpu.make_async_copy(out_ref.at[at], out_any.at[at], sems.at[piece])
                copy.start()
                copies.append(copy)
        for copy in copies:
            copy.wait()

    shape = (blocks_here, row_count, order)
    return pl.pallas_call(
        body,
        out_shape=jax.ShapeDtypeStruct(shape, slots.dtype),
        in_specs=[SMEM, VMEM, VMEM],
        out_specs=ANY,
        scratch_shapes=[
            pltpu.VMEM(shape, slots.dtype),
            pltpu.SemaphoreType.DMA((PIECES,)),
        ],
        compiler_params=params(4),
        name="scale_blocks",
    )(flags, row_norms, slots)


def refresh(flags, grad_block, left_stats, right_stats):
    order = grad_block.shape[0]
    strip = 64

    def body(flag_ref, grad_ref, left_ref, right_ref, left_out, right_out, done_ref, wide, low, first):
        def one(stat_ref, out_ref, dims):
            grad = grad_ref[...]
            wide[...] = lax.dot_general(grad, grad, dims, preferred_element_type=jnp.float32)

            def shift(i, total):
                at = pl.ds(i * strip, strip)
                on_diagonal = lax.broadcasted_iota(
                    jnp.int32, (strip, order), 1
                ) == i * strip + lax.broadcasted_iota(jnp.int32, (strip, order), 0)
                shifted = stat_decay * stat_ref[at] + wide[at] / order
                shifted = shifted + jnp.where(on_diagonal, ridge_term, 0.0)
                wide[at] = shifted
                return total + jnp.sum(
                    (shifted * shifted).reshape(strip // 8, 8, order), axis=0
                )

            squares = lax.fori_loop(
                0, order // strip, shift, jnp.zeros((8, order), jnp.float32)
            )
            scale = jnp.sqrt(jnp.sum(squares, keepdims=True) + tiny_term)
            start = 1.0 / jnp.sqrt(jnp.sqrt(scale))

            def begin(i, carry):
                at = pl.ds(i * strip, strip)
                on_diagonal = lax.broadcasted_iota(
                    jnp.int32, (strip, order), 1
                ) == i * strip + lax.broadcasted_iota(jnp.int32, (strip, order), 0)
                matrix = wide[at] / scale
                factor = ((jnp.where(on_diagonal, 5.0, 0.0) - matrix) / 4.0).astype(jnp.bfloat16)
                low[0, at] = matrix.astype(jnp.bfloat16)
                low[1, at] = factor
                first[at] = (start * factor.astype(jnp.float32)).astype(jnp.bfloat16)
                return carry

            lax.fori_loop(0, order // strip, begin, 0)

            def dot(a, b):
                return jnp.dot(a, b, preferred_element_type=jnp.float32)

            low[2] = dot(low[1], low[1]).astype(jnp.bfloat16)
            low[1] = dot(low[2], low[2]).astype(jnp.bfloat16)
            wide[...] = dot(low[1], low[0])

            def again(i, carry):
                at = pl.ds(i * strip, strip)
                on_diagonal = lax.broadcasted_iota(
                    jnp.int32, (strip, order), 1
                ) == i * strip + lax.broadcasted_iota(jnp.int32, (strip, order), 0)
                low[2, at] = ((jnp.where(on_diagonal, 5.0, 0.0) - wide[at]) / 4.0).astype(
                    jnp.bfloat16
                )
                return carry

            lax.fori_loop(0, order // strip, again, 0)
            out_ref[...] = dot(first[...], low[2]).astype(jnp.bfloat16)

        done_ref[0] = flag_ref[0]

        @pl.when(flag_ref[0] == 1)
        def _():
            one(left_ref, left_out, (((1,), (1,)), ((), ())))
            one(right_ref, right_out, (((0,), (0,)), ((), ())))

        @pl.when(flag_ref[0] == 0)
        def _():
            left_out[...] = jnp.zeros_like(left_out)
            right_out[...] = jnp.zeros_like(right_out)

    root = jax.ShapeDtypeStruct((order, order), jnp.bfloat16)
    return pl.pallas_call(
        body,
        out_shape=(root, root, pltpu.SMEM((1,), jnp.int32)),
        in_specs=[SMEM, VMEM, VMEM, VMEM],
        out_specs=(VMEM, VMEM, SMEM),
        scratch_shapes=[
            pltpu.VMEM((order, order), jnp.float32),
            pltpu.VMEM((3, order, order), jnp.bfloat16),
            pltpu.VMEM((order, order), jnp.bfloat16),
        ],
        compiler_params=params(24),
        name="refresh",
    )(flags, grad_block, left_stats, right_stats)


def shards(gradient, owners, left_stats, right_stats, left_roots_old, right_roots_old):
    dp_count = lax.axis_size(DP)
    mp_count = lax.axis_size(MP)
    blocks_here = gradient.shape[1]
    row_count = gradient.shape[2]
    block_width = gradient.shape[3]
    outgoing, flags = place_blocks(owners, gradient[0], dp_count)
    arrived = lax.all_to_all(outgoing, DP, split_axis=0, concat_axis=0, tiled=True)
    grad_block = arrived.reshape(dp_count * row_count, block_width)
    slots = precondition(
        flags, grad_block, left_roots_old[0, 0], right_roots_old[0, 0], blocks_here, row_count
    )
    returned = lax.all_to_all(slots, DP, split_axis=0, concat_axis=0, tiled=True)
    left_root, right_root, done = refresh(flags, grad_block, left_stats[0, 0], right_stats[0, 0])
    norms = add_norms(returned, done, mp_count)
    row_norms = lax.all_to_all(norms, MP, split_axis=0, concat_axis=0, tiled=True)
    update = scale_blocks(flags, row_norms, returned, row_count)[None]
    return (update, left_root[None, None], right_root[None, None])


def solution(mesh):
    finer = Mesh(
        mesh.devices.reshape(2, 2, 8, 2, 4, 2),
        ("dp_0h", "dp_0l", "dp_1", "dp_2", "mp_0", "mp_1"),
    )
    placed = (
        P(MP, None, DP, None),
        P(MP, None),
        P(MP, DP, None, None),
        P(MP, DP, None, None),
        P(MP, DP, None, None),
        P(MP, DP, None, None),
    )
    return jax.shard_map(
        shards,
        mesh=finer,
        in_specs=placed,
        out_specs=(P(MP, None, DP, None), P(MP, DP, None, None), P(MP, DP, None, None)),
        check_vma=False,
    )
```

```python
import jax
import jax.numpy as jnp
from jax import lax
from jax.experimental import pallas as pl
from jax.experimental.pallas import tpu as pltpu
from jax.sharding import Mesh
from jax.sharding import PartitionSpec as P

ITERS = 2
DP = ("dp_0h", "dp_0l", "dp_1", "dp_2")
MP = ("mp_0", "mp_1")
NEAR = ("dp_0h", "mp_0", "mp_1")
PAIRS = ("dp_0l", "dp_1", "dp_2")
LANES = 128
TILE = 4
PIECES = 4
MIB = 1024 * 1024
PLACE_MIB = 54


stat_decay = 0.9
ridge_term = 0.001
tiny_term = 1e-06

SMEM = pl.BlockSpec(memory_space=pltpu.SMEM)
VMEM = pl.BlockSpec(memory_space=pltpu.VMEM)
ANY = pl.BlockSpec(memory_space=pl.ANY)


def params(mib):
    return pltpu.CompilerParams(vmem_limit_bytes=mib * MIB)


def tiles_of(row_count, width):
    return [
        (slice(r, r + TILE), slice(c, c + LANES))
        for c in range(0, width, LANES)
        for r in range(0, row_count, TILE)
    ]


def partner_of(owner, dp_count):
    half = dp_count // 2
    return jnp.where(owner < half, owner + half, owner - half)


def place_blocks(owners, blocks, dp_count):
    blocks_here, row_count, width = blocks.shape
    per_piece = blocks_here // PIECES

    def body(owner_any, block_any, slot_ref, flag_ref, owner_ref, block_ref, sems):
        owner_fetch = pltpu.make_async_copy(owner_any, owner_ref, sems.at[PIECES])
        owner_fetch.start()
        fetches = []
        for piece in range(PIECES):
            at = pl.ds(piece * per_piece, per_piece)
            fetch = pltpu.make_async_copy(block_any.at[at], block_ref.at[at], sems.at[piece])
            fetch.start()
            fetches.append(fetch)
        owner_fetch.wait()
        my_index = lax.axis_index(DP)
        busy = jnp.int32(0)
        mine = jnp.int32(0)
        for j in range(blocks_here):
            if j % per_piece == 0:
                fetches[j // per_piece].wait()
            owner = owner_ref[0, j]
            rows = block_ref[j]
            slot_ref[owner] = rows
            slot_ref[partner_of(owner, dp_count)] = rows
            here = (owner == my_index).astype(jnp.int32)
            beside = (partner_of(owner, dp_count) == my_index).astype(jnp.int32)
            busy = busy + here
            mine = mine + (here + beside) * j
            flag_ref[2 + j] = owner
        flag_ref[0] = busy
        flag_ref[1] = mine

    return pl.pallas_call(
        body,
        out_shape=(
            pltpu.VMEM((dp_count, row_count, width), blocks.dtype),
            pltpu.SMEM((2 + blocks_here,), jnp.int32),
        ),
        in_specs=[ANY, ANY],
        out_specs=(VMEM, SMEM),
        scratch_shapes=[
            pltpu.SMEM(owners.shape, owners.dtype),
            pltpu.VMEM(blocks.shape, blocks.dtype),
            pltpu.SemaphoreType.DMA((PIECES + 1,)),
        ],
        compiler_params=params(PLACE_MIB),
        name="place_blocks",
    )(owners, blocks)


def precondition(flags, grad_block, left, right, blocks_here, near_count, row_count):
    order = grad_block.shape[0]
    half = order // 2
    slots = half // row_count
    strip = 128

    def body(flag_ref, grad_ref, left_ref, right_ref, stay_ref, pass_ref, norm_ref):
        def squares_of(total, rows):
            wide = rows.astype(jnp.float32)
            return total + jnp.sum((wide * wide).reshape(strip // 8, 8, order), axis=0)

        def write_norm(lane_of, total):
            lane = lax.broadcasted_iota(jnp.int32, (1, LANES), 1)
            row = jnp.where(lane == lane_of, jnp.sum(total, keepdims=True), 0.0)
            norm_ref[...] = jnp.broadcast_to(row[None], norm_ref.shape)

        @pl.when(flag_ref[0] == 1)
        def _():
            shaded = jnp.dot(grad_ref[...], right_ref[...], preferred_element_type=jnp.float32)
            shaded = shaded.astype(jnp.bfloat16)
            total = jnp.zeros((8, order), jnp.float32)
            here = lax.axis_index("dp_0h")
            for which, out_ref in ((1 - here, pass_ref), (here, stay_ref)):
                for i in range(half // strip):
                    first = pl.multiple_of(which * half + i * strip, strip)
                    rows = jnp.dot(
                        left_ref[pl.ds(first, strip)], shaded, preferred_element_type=jnp.float32
                    ).astype(jnp.bfloat16)
                    at = slice(i * strip // row_count, (i + 1) * strip // row_count)
                    out_ref[at] = rows.reshape(strip // row_count, row_count, order)
                    total = squares_of(total, rows)
            write_norm(flag_ref[1] + blocks_here, total)

        @pl.when(flag_ref[0] == 0)
        def _():
            total = jnp.zeros((8, order), jnp.float32)
            for i in range(order // strip):
                total = squares_of(total, grad_ref[i * strip : (i + 1) * strip])
            write_norm(flag_ref[1], total)

    return pl.pallas_call(
        body,
        out_shape=(
            pltpu.VMEM((slots, row_count, order), jnp.bfloat16),
            pltpu.VMEM((slots, row_count, order), jnp.bfloat16),
            pltpu.VMEM((near_count, 1, LANES), jnp.float32),
        ),
        in_specs=[SMEM, VMEM, VMEM, VMEM],
        out_specs=(VMEM, VMEM, VMEM),
        compiler_params=params(12),
        name="precondition",
    )(flags, grad_block, left, right)


def fill_slots(flags, near_norms, passed, stays):
    slot_count, row_count, order = stays.shape
    tiles = row_count * order // (TILE * LANES)
    per_piece = slot_count // PIECES

    def body(flag_ref, norm_ref, passed_ref, stay_ref, out_any, out_ref, sems):
        total = jnp.sum(norm_ref[...], axis=0)
        high = total.astype(jnp.bfloat16).astype(jnp.float32)
        rest = total - high
        middle = rest.astype(jnp.bfloat16).astype(jnp.float32)
        low = rest - middle
        shape = (TILE, LANES)
        row = lax.broadcasted_iota(jnp.int32, shape, 0)
        packed = jnp.where(
            row == 0,
            jnp.broadcast_to(high, shape),
            jnp.where(
                row == 1,
                jnp.broadcast_to(middle, shape),
                jnp.where(row == 2, jnp.broadcast_to(low, shape), 0.0),
            ),
        ).astype(jnp.bfloat16)

        def fill(rows_ref):
            copies = []
            for piece in range(PIECES):
                at = pl.ds(piece * per_piece, per_piece)
                out_ref[at, tiles] = jnp.broadcast_to(packed[None], (per_piece, TILE, LANES))
                for t, (rows, lanes) in enumerate(tiles_of(row_count, order)):
                    out_ref[at, t] = rows_ref[at, rows, lanes]
                copy = pltpu.make_async_copy(out_ref.at[at], out_any.at[at], sems.at[piece])
                copy.start()
                copies.append(copy)
            for copy in copies:
                copy.wait()

        @pl.when(flag_ref[0] == 1)
        def _():
            fill(stay_ref)

        @pl.when(flag_ref[0] == 0)
        def _():
            fill(passed_ref)

    return pl.pallas_call(
        body,
        out_shape=jax.ShapeDtypeStruct((slot_count, tiles + 1, TILE, LANES), stays.dtype),
        in_specs=[SMEM, VMEM, VMEM, VMEM],
        out_specs=ANY,
        scratch_shapes=[
            pltpu.VMEM((slot_count, tiles + 1, TILE, LANES), stays.dtype),
            pltpu.SemaphoreType.DMA((PIECES,)),
        ],
        compiler_params=params(4),
        name="fill_slots",
    )(flags, near_norms, passed, stays)


def scale_blocks(flags, slots, row_count):
    blocks_here = flags.shape[0] - 2
    slot_count = slots.shape[0]
    tiles = slots.shape[1] - 1
    order = tiles * TILE * LANES // row_count
    per_piece = blocks_here // PIECES

    def body(flag_ref, slot_ref, out_any, out_ref, sems):
        copies = []
        norms = jnp.sum(slot_ref[:, tiles].astype(jnp.float32), axis=0)
        totals = norms[0:1] + (norms[1:2] + norms[2:3])
        columns = jnp.broadcast_to(totals, (LANES, LANES)).T
        ratio = jnp.sqrt(
            columns[:blocks_here] / (columns[blocks_here : 2 * blocks_here] + tiny_term)
        )
        for j in range(blocks_here):
            owner = flag_ref[2 + j]
            scale = jnp.broadcast_to(ratio[j : j + 1], (TILE, LANES))
            slot = jnp.where(owner < slot_count, owner, owner - slot_count)
            for t, (rows, lanes) in enumerate(tiles_of(row_count, order)):
                tile = slot_ref[slot, t].astype(jnp.float32)
                out_ref[j, rows, lanes] = (scale * tile).astype(out_ref.dtype)
            if (j + 1) % per_piece == 0:
                piece = j // per_piece
                at = pl.ds(piece * per_piece, per_piece)
                copy = pltpu.make_async_copy(out_ref.at[at], out_any.at[at], sems.at[piece])
                copy.start()
                copies.append(copy)
        for copy in copies:
            copy.wait()

    return pl.pallas_call(
        body,
        out_shape=jax.ShapeDtypeStruct((blocks_here, row_count, order), slots.dtype),
        in_specs=[SMEM, VMEM],
        out_specs=ANY,
        scratch_shapes=[
            pltpu.VMEM((blocks_here, row_count, order), slots.dtype),
            pltpu.SemaphoreType.DMA((PIECES,)),
        ],
        compiler_params=params(4),
        name="scale_blocks",
    )(flags, slots)


def refresh(flags, grad_block, left_stats, right_stats):
    order = grad_block.shape[0]
    strip = 64

    def body(flag_ref, grad_ref, left_ref, right_ref, left_out, right_out, wide, low, first):
        def one(stat_ref, out_ref, dims):
            grad = grad_ref[...]
            wide[...] = lax.dot_general(grad, grad, dims, preferred_element_type=jnp.float32)

            def shift(i, total):
                at = pl.ds(i * strip, strip)
                on_diagonal = lax.broadcasted_iota(
                    jnp.int32, (strip, order), 1
                ) == i * strip + lax.broadcasted_iota(jnp.int32, (strip, order), 0)
                shifted = stat_decay * stat_ref[at] + wide[at] / order
                shifted = shifted + jnp.where(on_diagonal, ridge_term, 0.0)
                wide[at] = shifted
                return total + jnp.sum(
                    (shifted * shifted).reshape(strip // 8, 8, order), axis=0
                )

            squares = lax.fori_loop(
                0, order // strip, shift, jnp.zeros((8, order), jnp.float32)
            )
            scale = jnp.sqrt(jnp.sum(squares, keepdims=True) + tiny_term)
            start = 1.0 / jnp.sqrt(jnp.sqrt(scale))

            def begin(i, carry):
                at = pl.ds(i * strip, strip)
                on_diagonal = lax.broadcasted_iota(
                    jnp.int32, (strip, order), 1
                ) == i * strip + lax.broadcasted_iota(jnp.int32, (strip, order), 0)
                matrix = wide[at] / scale
                factor = ((jnp.where(on_diagonal, 5.0, 0.0) - matrix) / 4.0).astype(jnp.bfloat16)
                low[0, at] = matrix.astype(jnp.bfloat16)
                low[1, at] = factor
                first[at] = (start * factor.astype(jnp.float32)).astype(jnp.bfloat16)
                return carry

            lax.fori_loop(0, order // strip, begin, 0)

            def dot(a, b):
                return jnp.dot(a, b, preferred_element_type=jnp.float32)

            low[2] = dot(low[1], low[1]).astype(jnp.bfloat16)
            low[1] = dot(low[2], low[2]).astype(jnp.bfloat16)
            wide[...] = dot(low[1], low[0])

            def again(i, carry):
                at = pl.ds(i * strip, strip)
                on_diagonal = lax.broadcasted_iota(
                    jnp.int32, (strip, order), 1
                ) == i * strip + lax.broadcasted_iota(jnp.int32, (strip, order), 0)
                low[2, at] = ((jnp.where(on_diagonal, 5.0, 0.0) - wide[at]) / 4.0).astype(
                    jnp.bfloat16
                )
                return carry

            lax.fori_loop(0, order // strip, again, 0)
            out_ref[...] = dot(first[...], low[2]).astype(jnp.bfloat16)

        @pl.when(flag_ref[0] == 1)
        def _():
            one(left_ref, left_out, (((1,), (1,)), ((), ())))
            one(right_ref, right_out, (((0,), (0,)), ((), ())))

        @pl.when(flag_ref[0] == 0)
        def _():
            left_out[...] = jnp.zeros_like(left_out)
            right_out[...] = jnp.zeros_like(right_out)

    root = jax.ShapeDtypeStruct((order, order), jnp.bfloat16)
    return pl.pallas_call(
        body,
        out_shape=(root, root),
        in_specs=[SMEM, VMEM, VMEM, VMEM],
        out_specs=(VMEM, VMEM),
        scratch_shapes=[
            pltpu.VMEM((order, order), jnp.float32),
            pltpu.VMEM((3, order, order), jnp.bfloat16),
            pltpu.VMEM((order, order), jnp.bfloat16),
        ],
        compiler_params=params(24),
        name="refresh",
    )(flags, grad_block, left_stats, right_stats)


def shards(gradient, owners, left_stats, right_stats, left_roots_old, right_roots_old):
    dp_count = lax.axis_size(DP)
    near_count = lax.axis_size(NEAR)
    blocks_here = gradient.shape[1]
    row_count = gradient.shape[2]
    block_width = gradient.shape[3]
    outgoing, flags = place_blocks(owners, gradient[0], dp_count)
    arrived = lax.all_to_all(outgoing, DP, split_axis=0, concat_axis=0, tiled=True)
    grad_block = arrived.reshape(dp_count * row_count, block_width)
    stays, passes, norms = precondition(
        flags, grad_block, left_roots_old[0, 0], right_roots_old[0, 0], blocks_here, near_count, row_count
    )
    passed = lax.ppermute(passes, "dp_0h", [(0, 1), (1, 0)])
    near_norms = lax.all_to_all(norms, NEAR, split_axis=0, concat_axis=0, tiled=True)
    slots = fill_slots(flags, near_norms, passed, stays)
    returned = lax.all_to_all(slots, PAIRS, split_axis=0, concat_axis=0, tiled=True)
    left_root, right_root = refresh(flags, grad_block, left_stats[0, 0], right_stats[0, 0])
    update = scale_blocks(flags, returned, row_count)[None]
    return (update, left_root[None, None], right_root[None, None])


def solution(mesh):
    finer = Mesh(
        mesh.devices.reshape(2, 2, 8, 2, 4, 2),
        ("dp_0h", "dp_0l", "dp_1", "dp_2", "mp_0", "mp_1"),
    )
    placed = (
        P(MP, None, DP, None),
        P(MP, None),
        P(MP, DP, None, None),
        P(MP, DP, None, None),
        P(MP, DP, None, None),
        P(MP, DP, None, None),
    )
    return jax.shard_map(
        shards,
        mesh=finer,
        in_specs=placed,
        out_specs=(P(MP, None, DP, None), P(MP, DP, None, None), P(MP, DP, None, None)),
        check_vma=False,
    )
```

```python
import jax
import jax.numpy as jnp
from jax import lax
from jax.experimental import pallas as pl
from jax.experimental.pallas import tpu as pltpu
from jax.sharding import Mesh
from jax.sharding import PartitionSpec as P

ITERS = 2
DP = ("dp_0h", "dp_0l", "dp_1", "dp_2")
MP = ("mp_0", "mp_1")
LANES = 128
TILE = 4
PIECES = 4
CHAINS = 8
MIB = 1024 * 1024
PLACE_MIB = 54


stat_decay = 0.9
ridge_term = 0.001
tiny_term = 1e-06

SMEM = pl.BlockSpec(memory_space=pltpu.SMEM)
VMEM = pl.BlockSpec(memory_space=pltpu.VMEM)
ANY = pl.BlockSpec(memory_space=pl.ANY)


def params(mib):
    return pltpu.CompilerParams(vmem_limit_bytes=mib * MIB)


def tiles_of(row_count, width):
    return [
        (slice(r, r + TILE), slice(c, c + LANES))
        for c in range(0, width, LANES)
        for r in range(0, row_count, TILE)
    ]


def partner_of(owner, dp_count):
    half = dp_count // 2
    return jnp.where(owner < half, owner + half, owner - half)


def place_blocks(owners, blocks, dp_count):
    blocks_here, row_count, width = blocks.shape
    per_piece = blocks_here // PIECES

    def body(owner_any, block_any, slot_ref, flag_ref, owner_ref, block_ref, sems):
        owner_fetch = pltpu.make_async_copy(owner_any, owner_ref, sems.at[PIECES])
        owner_fetch.start()
        fetches = []
        for piece in range(PIECES):
            at = pl.ds(piece * per_piece, per_piece)
            fetch = pltpu.make_async_copy(block_any.at[at], block_ref.at[at], sems.at[piece])
            fetch.start()
            fetches.append(fetch)
        owner_fetch.wait()
        my_index = lax.axis_index(DP)
        busy = jnp.int32(0)
        mine = jnp.int32(0)
        for j in range(blocks_here):
            if j % per_piece == 0:
                fetches[j // per_piece].wait()
            owner = owner_ref[0, j]
            rows = block_ref[j]
            slot_ref[owner] = rows
            slot_ref[partner_of(owner, dp_count)] = rows
            here = (owner == my_index).astype(jnp.int32)
            beside = (partner_of(owner, dp_count) == my_index).astype(jnp.int32)
            busy = busy + here
            mine = mine + (here + beside) * j
            flag_ref[2 + j] = owner
        flag_ref[0] = busy
        flag_ref[1] = mine

    return pl.pallas_call(
        body,
        out_shape=(
            pltpu.VMEM((dp_count, row_count, width), blocks.dtype),
            pltpu.SMEM((2 + blocks_here,), jnp.int32),
        ),
        in_specs=[ANY, ANY],
        out_specs=(VMEM, SMEM),
        scratch_shapes=[
            pltpu.SMEM(owners.shape, owners.dtype),
            pltpu.VMEM(blocks.shape, blocks.dtype),
            pltpu.SemaphoreType.DMA((PIECES + 1,)),
        ],
        compiler_params=params(PLACE_MIB),
        name="place_blocks",
    )(owners, blocks)


def precondition(flags, grad_block, left, right, blocks_here, mp_count, row_count):
    order = grad_block.shape[0]
    half = order // 2
    slots = order // row_count
    strip = 128

    def body(flag_ref, grad_ref, left_ref, right_ref, stay_ref, pass_ref, norm_ref):
        def squares_of(total, rows):
            wide = rows.astype(jnp.float32)
            return total + jnp.sum((wide * wide).reshape(strip // 8, 8, order), axis=0)

        def write_norm(lane_of, total):
            lane = lax.broadcasted_iota(jnp.int32, (1, LANES), 1)
            row = jnp.where(lane == lane_of, jnp.sum(total, keepdims=True), 0.0)
            norm_ref[...] = jnp.broadcast_to(row[None], norm_ref.shape)

        @pl.when(flag_ref[0] == 1)
        def _():
            shaded = jnp.dot(grad_ref[...], right_ref[...], preferred_element_type=jnp.float32)
            shaded = shaded.astype(jnp.bfloat16)
            total = jnp.zeros((8, order), jnp.float32)
            for i in range(order // strip):
                rows = jnp.dot(
                    left_ref[i * strip : (i + 1) * strip], shaded, preferred_element_type=jnp.float32
                ).astype(jnp.bfloat16)
                at = slice(i * strip // row_count, (i + 1) * strip // row_count)
                stay_ref[at] = rows[:, :half].reshape(strip // row_count, row_count, half)
                pass_ref[at] = rows[:, half:].reshape(strip // row_count, row_count, half)
                total = squares_of(total, rows)
            write_norm(flag_ref[1] + blocks_here, total)

        @pl.when(flag_ref[0] == 0)
        def _():
            total = jnp.zeros((8, order), jnp.float32)
            for i in range(order // strip):
                total = squares_of(total, grad_ref[i * strip : (i + 1) * strip])
            write_norm(flag_ref[1], total)

    return pl.pallas_call(
        body,
        out_shape=(
            pltpu.VMEM((slots, row_count, half), jnp.bfloat16),
            pltpu.VMEM((slots, row_count, half), jnp.bfloat16),
            pltpu.VMEM((mp_count, 1, LANES), jnp.float32),
        ),
        in_specs=[SMEM, VMEM, VMEM, VMEM],
        out_specs=(VMEM, VMEM, VMEM),
        compiler_params=params(12),
        name="precondition",
    )(flags, grad_block, left, right)


def fill_slots(flags, row_norms, passed, stays):
    slot_count, row_count, half = stays.shape
    tiles = row_count * half // (TILE * LANES)
    per_piece = slot_count // PIECES

    def body(flag_ref, norm_ref, passed_ref, stay_ref, out_any, out_ref, sems):
        def piece_copy(piece):
            at = (pl.ds(piece * per_piece, per_piece), pl.ds(0, tiles))
            return pltpu.make_async_copy(out_ref.at[at], out_any.at[at], sems.at[piece])

        def fill(rows_ref):
            for piece in range(PIECES):
                at = pl.ds(piece * per_piece, per_piece)
                for t, (rows, lanes) in enumerate(tiles_of(row_count, half)):
                    out_ref[at, t] = rows_ref[at, rows, lanes]
                piece_copy(piece).start()

        @pl.when(flag_ref[0] == 1)
        def _():
            fill(stay_ref)

        @pl.when(flag_ref[0] == 0)
        def _():
            fill(passed_ref)

        total = jnp.sum(norm_ref[...], axis=0)
        high = total.astype(jnp.bfloat16).astype(jnp.float32)
        rest = total - high
        middle = rest.astype(jnp.bfloat16).astype(jnp.float32)
        low = rest - middle
        shape = (TILE, LANES)
        row = lax.broadcasted_iota(jnp.int32, shape, 0)
        packed = jnp.where(
            row == 0,
            jnp.broadcast_to(high, shape),
            jnp.where(
                row == 1,
                jnp.broadcast_to(middle, shape),
                jnp.where(row == 2, jnp.broadcast_to(low, shape), 0.0),
            ),
        ).astype(jnp.bfloat16)
        out_ref[:, tiles] = jnp.broadcast_to(packed[None], (slot_count, TILE, LANES))
        norm_copy = pltpu.make_async_copy(out_ref.at[:, tiles], out_any.at[:, tiles], sems.at[PIECES])
        norm_copy.start()
        for piece in range(PIECES):
            piece_copy(piece).wait()
        norm_copy.wait()

    return pl.pallas_call(
        body,
        out_shape=jax.ShapeDtypeStruct((slot_count, tiles + 1, TILE, LANES), stays.dtype),
        in_specs=[SMEM, VMEM, VMEM, VMEM],
        out_specs=ANY,
        scratch_shapes=[
            pltpu.VMEM((slot_count, tiles + 1, TILE, LANES), stays.dtype),
            pltpu.SemaphoreType.DMA((PIECES + 1,)),
        ],
        compiler_params=params(4),
        name="fill_slots",
    )(flags, row_norms, passed, stays)


def scale_blocks(flags, slots, row_count):
    blocks_here = flags.shape[0] - 2
    slot_count = slots.shape[0]
    tiles = slots.shape[1] - 1
    half = tiles * TILE * LANES // row_count
    per_piece = blocks_here // PIECES

    def body(flag_ref, slot_ref, out_any, out_ref, sems):
        copies = []
        chains = [slot_ref[p, tiles].astype(jnp.float32) for p in range(CHAINS)]
        for p in range(CHAINS, slot_count):
            chains[p % CHAINS] = chains[p % CHAINS] + slot_ref[p, tiles].astype(jnp.float32)
        while len(chains) > 1:
            chains = [one + two for one, two in zip(chains[::2], chains[1::2])]
        norms = chains[0]
        totals = norms[0:1] + (norms[1:2] + norms[2:3])
        columns = jnp.broadcast_to(totals, (LANES, LANES)).T
        ratio = jnp.sqrt(
            columns[:blocks_here] / (columns[blocks_here : 2 * blocks_here] + tiny_term)
        )
        for j in range(blocks_here):
            owner = flag_ref[2 + j]
            scale = jnp.broadcast_to(ratio[j : j + 1], (TILE, LANES))
            for k, slot in enumerate((owner, partner_of(owner, slot_count))):
                for t, (rows, lanes) in enumerate(tiles_of(row_count, half)):
                    at = slice(k * half + lanes.start, k * half + lanes.stop)
                    tile = slot_ref[slot, t].astype(jnp.float32)
                    out_ref[j, rows, at] = (scale * tile).astype(out_ref.dtype)
            if (j + 1) % per_piece == 0:
                piece = j // per_piece
                at = pl.ds(piece * per_piece, per_piece)
                copy = pltpu.make_async_copy(out_ref.at[at], out_any.at[at], sems.at[piece])
                copy.start()
                copies.append(copy)
        for copy in copies:
            copy.wait()

    return pl.pallas_call(
        body,
        out_shape=jax.ShapeDtypeStruct((blocks_here, row_count, 2 * half), slots.dtype),
        in_specs=[SMEM, VMEM],
        out_specs=ANY,
        scratch_shapes=[
            pltpu.VMEM((blocks_here, row_count, 2 * half), slots.dtype),
            pltpu.SemaphoreType.DMA((PIECES,)),
        ],
        compiler_params=params(4),
        name="scale_blocks",
    )(flags, slots)


def refresh(flags, grad_block, left_stats, right_stats):
    order = grad_block.shape[0]
    strip = 64

    def body(flag_ref, grad_ref, left_ref, right_ref, left_out, right_out, wide, low, first):
        def one(stat_ref, out_ref, dims):
            grad = grad_ref[...]
            wide[...] = lax.dot_general(grad, grad, dims, preferred_element_type=jnp.float32)

            def shift(i, total):
                at = pl.ds(i * strip, strip)
                on_diagonal = lax.broadcasted_iota(
                    jnp.int32, (strip, order), 1
                ) == i * strip + lax.broadcasted_iota(jnp.int32, (strip, order), 0)
                shifted = stat_decay * stat_ref[at] + wide[at] / order
                shifted = shifted + jnp.where(on_diagonal, ridge_term, 0.0)
                wide[at] = shifted
                return total + jnp.sum(
                    (shifted * shifted).reshape(strip // 8, 8, order), axis=0
                )

            squares = lax.fori_loop(
                0, order // strip, shift, jnp.zeros((8, order), jnp.float32)
            )
            scale = jnp.sqrt(jnp.sum(squares, keepdims=True) + tiny_term)
            start = 1.0 / jnp.sqrt(jnp.sqrt(scale))

            def begin(i, carry):
                at = pl.ds(i * strip, strip)
                on_diagonal = lax.broadcasted_iota(
                    jnp.int32, (strip, order), 1
                ) == i * strip + lax.broadcasted_iota(jnp.int32, (strip, order), 0)
                matrix = wide[at] / scale
                factor = ((jnp.where(on_diagonal, 5.0, 0.0) - matrix) / 4.0).astype(jnp.bfloat16)
                low[0, at] = matrix.astype(jnp.bfloat16)
                low[1, at] = factor
                first[at] = (start * factor.astype(jnp.float32)).astype(jnp.bfloat16)
                return carry

            lax.fori_loop(0, order // strip, begin, 0)

            def dot(a, b):
                return jnp.dot(a, b, preferred_element_type=jnp.float32)

            low[2] = dot(low[1], low[1]).astype(jnp.bfloat16)
            low[1] = dot(low[2], low[2]).astype(jnp.bfloat16)
            wide[...] = dot(low[1], low[0])

            def again(i, carry):
                at = pl.ds(i * strip, strip)
                on_diagonal = lax.broadcasted_iota(
                    jnp.int32, (strip, order), 1
                ) == i * strip + lax.broadcasted_iota(jnp.int32, (strip, order), 0)
                low[2, at] = ((jnp.where(on_diagonal, 5.0, 0.0) - wide[at]) / 4.0).astype(
                    jnp.bfloat16
                )
                return carry

            lax.fori_loop(0, order // strip, again, 0)
            out_ref[...] = dot(first[...], low[2]).astype(jnp.bfloat16)

        @pl.when(flag_ref[0] == 1)
        def _():
            one(left_ref, left_out, (((1,), (1,)), ((), ())))
            one(right_ref, right_out, (((0,), (0,)), ((), ())))

        @pl.when(flag_ref[0] == 0)
        def _():
            left_out[...] = jnp.zeros_like(left_out)
            right_out[...] = jnp.zeros_like(right_out)

    root = jax.ShapeDtypeStruct((order, order), jnp.bfloat16)
    return pl.pallas_call(
        body,
        out_shape=(root, root),
        in_specs=[SMEM, VMEM, VMEM, VMEM],
        out_specs=(VMEM, VMEM),
        scratch_shapes=[
            pltpu.VMEM((order, order), jnp.float32),
            pltpu.VMEM((3, order, order), jnp.bfloat16),
            pltpu.VMEM((order, order), jnp.bfloat16),
        ],
        compiler_params=params(24),
        name="refresh",
    )(flags, grad_block, left_stats, right_stats)


def shards(gradient, owners, left_stats, right_stats, left_roots_old, right_roots_old):
    dp_count = lax.axis_size(DP)
    mp_count = lax.axis_size(MP)
    blocks_here = gradient.shape[1]
    row_count = gradient.shape[2]
    block_width = gradient.shape[3]
    outgoing, flags = place_blocks(owners, gradient[0], dp_count)
    arrived = lax.all_to_all(outgoing, DP, split_axis=0, concat_axis=0, tiled=True)
    grad_block = arrived.reshape(dp_count * row_count, block_width)
    stays, passes, norms = precondition(
        flags, grad_block, left_roots_old[0, 0], right_roots_old[0, 0], blocks_here, mp_count, row_count
    )
    passed = lax.ppermute(passes, "dp_0h", [(0, 1), (1, 0)])
    row_norms = lax.all_to_all(norms, MP, split_axis=0, concat_axis=0, tiled=True)
    slots = fill_slots(flags, row_norms, passed, stays)
    returned = lax.all_to_all(slots, DP, split_axis=0, concat_axis=0, tiled=True)
    left_root, right_root = refresh(flags, grad_block, left_stats[0, 0], right_stats[0, 0])
    update = scale_blocks(flags, returned, row_count)[None]
    return (update, left_root[None, None], right_root[None, None])


def solution(mesh):
    finer = Mesh(
        mesh.devices.reshape(2, 2, 8, 2, 4, 2),
        ("dp_0h", "dp_0l", "dp_1", "dp_2", "mp_0", "mp_1"),
    )
    placed = (
        P(MP, None, DP, None),
        P(MP, None),
        P(MP, DP, None, None),
        P(MP, DP, None, None),
        P(MP, DP, None, None),
        P(MP, DP, None, None),
    )
    return jax.shard_map(
        shards,
        mesh=finer,
        in_specs=placed,
        out_specs=(P(MP, None, DP, None), P(MP, DP, None, None), P(MP, DP, None, None)),
        check_vma=False,
    )
```

```python
import jax
import jax.numpy as jnp
from jax import lax
from jax.experimental import pallas as pl
from jax.experimental.pallas import tpu as pltpu
from jax.sharding import Mesh
from jax.sharding import PartitionSpec as P

ITERS = 2
DP = ("dp_0h", "dp_0l", "dp_1", "dp_2")
MP = ("mp_0", "mp_1")
LANES = 128
TILE = 4
PIECES = 8
CHAINS = 8
MIB = 1024 * 1024
PLACE_MIB = 54


stat_decay = 0.9
ridge_term = 0.001
tiny_term = 1e-06

SMEM = pl.BlockSpec(memory_space=pltpu.SMEM)
VMEM = pl.BlockSpec(memory_space=pltpu.VMEM)
ANY = pl.BlockSpec(memory_space=pl.ANY)


def params(mib):
    return pltpu.CompilerParams(vmem_limit_bytes=mib * MIB)


def tiles_of(row_count, width):
    return [
        (slice(r, r + TILE), slice(c, c + LANES))
        for c in range(0, width, LANES)
        for r in range(0, row_count, TILE)
    ]


def partner_of(owner, dp_count):
    half = dp_count // 2
    return jnp.where(owner < half, owner + half, owner - half)


def place_blocks(owners, blocks, dp_count):
    blocks_here, row_count, width = blocks.shape
    per_piece = blocks_here // PIECES

    def body(owner_any, block_any, slot_ref, flag_ref, owner_ref, block_ref, sems):
        owner_fetch = pltpu.make_async_copy(owner_any, owner_ref, sems.at[PIECES])
        owner_fetch.start()
        fetches = []
        for piece in range(PIECES):
            at = pl.ds(piece * per_piece, per_piece)
            fetch = pltpu.make_async_copy(block_any.at[at], block_ref.at[at], sems.at[piece])
            fetch.start()
            fetches.append(fetch)
        owner_fetch.wait()
        my_index = lax.axis_index(DP)
        busy = jnp.int32(0)
        mine = jnp.int32(0)
        for j in range(blocks_here):
            if j % per_piece == 0:
                fetches[j // per_piece].wait()
            owner = owner_ref[0, j]
            rows = block_ref[j]
            slot_ref[owner] = rows
            slot_ref[partner_of(owner, dp_count)] = rows
            here = (owner == my_index).astype(jnp.int32)
            beside = (partner_of(owner, dp_count) == my_index).astype(jnp.int32)
            busy = busy + here
            mine = mine + (here + beside) * j
            flag_ref[2 + j] = owner
        flag_ref[0] = busy
        flag_ref[1] = mine

    return pl.pallas_call(
        body,
        out_shape=(
            pltpu.VMEM((dp_count, row_count, width), blocks.dtype),
            pltpu.SMEM((2 + blocks_here,), jnp.int32),
        ),
        in_specs=[ANY, ANY],
        out_specs=(VMEM, SMEM),
        scratch_shapes=[
            pltpu.SMEM(owners.shape, owners.dtype),
            pltpu.VMEM(blocks.shape, blocks.dtype),
            pltpu.SemaphoreType.DMA((PIECES + 1,)),
        ],
        compiler_params=params(PLACE_MIB),
        name="place_blocks",
    )(owners, blocks)


def precondition(flags, grad_block, left, right, blocks_here, mp_count, row_count):
    order = grad_block.shape[0]
    half = order // 2
    slots = order // row_count
    strip = 128

    def body(flag_ref, grad_ref, left_ref, right_ref, stay_ref, pass_ref, norm_ref):
        def squares_of(total, rows):
            wide = rows.astype(jnp.float32)
            return total + jnp.sum((wide * wide).reshape(strip // 8, 8, order), axis=0)

        def write_norm(lane_of, total):
            lane = lax.broadcasted_iota(jnp.int32, (1, LANES), 1)
            row = jnp.where(lane == lane_of, jnp.sum(total, keepdims=True), 0.0)
            norm_ref[...] = jnp.broadcast_to(row[None], norm_ref.shape)

        @pl.when(flag_ref[0] == 1)
        def _():
            shaded = jnp.dot(grad_ref[...], right_ref[...], preferred_element_type=jnp.float32)
            shaded = shaded.astype(jnp.bfloat16)
            total = jnp.zeros((8, order), jnp.float32)
            for i in range(order // strip):
                rows = jnp.dot(
                    left_ref[i * strip : (i + 1) * strip], shaded, preferred_element_type=jnp.float32
                ).astype(jnp.bfloat16)
                at = slice(i * strip // row_count, (i + 1) * strip // row_count)
                stay_ref[at] = rows[:, :half].reshape(strip // row_count, row_count, half)
                pass_ref[at] = rows[:, half:].reshape(strip // row_count, row_count, half)
                total = squares_of(total, rows)
            write_norm(flag_ref[1] + blocks_here, total)

        @pl.when(flag_ref[0] == 0)
        def _():
            total = jnp.zeros((8, order), jnp.float32)
            for i in range(order // strip):
                total = squares_of(total, grad_ref[i * strip : (i + 1) * strip])
            write_norm(flag_ref[1], total)

    return pl.pallas_call(
        body,
        out_shape=(
            pltpu.VMEM((slots, row_count, half), jnp.bfloat16),
            pltpu.VMEM((slots, row_count, half), jnp.bfloat16),
            pltpu.VMEM((mp_count, 1, LANES), jnp.float32),
        ),
        in_specs=[SMEM, VMEM, VMEM, VMEM],
        out_specs=(VMEM, VMEM, VMEM),
        compiler_params=params(12),
        name="precondition",
    )(flags, grad_block, left, right)


def fill_slots(flags, row_norms, passed, stays):
    slot_count, row_count, half = stays.shape
    tiles = row_count * half // (TILE * LANES)
    per_piece = slot_count // PIECES

    def body(flag_ref, norm_ref, passed_ref, stay_ref, out_any, out_ref, sems):
        def piece_copy(piece):
            at = (pl.ds(piece * per_piece, per_piece), pl.ds(0, tiles))
            return pltpu.make_async_copy(out_ref.at[at], out_any.at[at], sems.at[piece])

        def fill(rows_ref):
            for piece in range(PIECES):
                at = pl.ds(piece * per_piece, per_piece)
                for t, (rows, lanes) in enumerate(tiles_of(row_count, half)):
                    out_ref[at, t] = rows_ref[at, rows, lanes]
                piece_copy(piece).start()

        @pl.when(flag_ref[0] == 1)
        def _():
            fill(stay_ref)

        @pl.when(flag_ref[0] == 0)
        def _():
            fill(passed_ref)

        total = jnp.sum(norm_ref[...], axis=0)
        high = total.astype(jnp.bfloat16).astype(jnp.float32)
        rest = total - high
        middle = rest.astype(jnp.bfloat16).astype(jnp.float32)
        low = rest - middle
        shape = (TILE, LANES)
        row = lax.broadcasted_iota(jnp.int32, shape, 0)
        packed = jnp.where(
            row == 0,
            jnp.broadcast_to(high, shape),
            jnp.where(
                row == 1,
                jnp.broadcast_to(middle, shape),
                jnp.where(row == 2, jnp.broadcast_to(low, shape), 0.0),
            ),
        ).astype(jnp.bfloat16)
        out_ref[:, tiles] = jnp.broadcast_to(packed[None], (slot_count, TILE, LANES))
        norm_copy = pltpu.make_async_copy(out_ref.at[:, tiles], out_any.at[:, tiles], sems.at[PIECES])
        norm_copy.start()
        for piece in range(PIECES):
            piece_copy(piece).wait()
        norm_copy.wait()

    return pl.pallas_call(
        body,
        out_shape=jax.ShapeDtypeStruct((slot_count, tiles + 1, TILE, LANES), stays.dtype),
        in_specs=[SMEM, VMEM, VMEM, VMEM],
        out_specs=ANY,
        scratch_shapes=[
            pltpu.VMEM((slot_count, tiles + 1, TILE, LANES), stays.dtype),
            pltpu.SemaphoreType.DMA((PIECES + 1,)),
        ],
        compiler_params=params(4),
        name="fill_slots",
    )(flags, row_norms, passed, stays)


def scale_blocks(flags, slots, row_count):
    blocks_here = flags.shape[0] - 2
    slot_count = slots.shape[0]
    tiles = slots.shape[1] - 1
    half = tiles * TILE * LANES // row_count
    per_piece = blocks_here // PIECES

    def body(flag_ref, slot_ref, out_any, out_ref, sems):
        copies = []
        chains = [slot_ref[p, tiles].astype(jnp.float32) for p in range(CHAINS)]
        for p in range(CHAINS, slot_count):
            chains[p % CHAINS] = chains[p % CHAINS] + slot_ref[p, tiles].astype(jnp.float32)
        while len(chains) > 1:
            chains = [one + two for one, two in zip(chains[::2], chains[1::2])]
        norms = chains[0]
        totals = norms[0:1] + (norms[1:2] + norms[2:3])
        columns = jnp.broadcast_to(totals, (LANES, LANES)).T
        ratio = jnp.sqrt(
            columns[:blocks_here] / (columns[blocks_here : 2 * blocks_here] + tiny_term)
        )
        for j in range(blocks_here):
            owner = flag_ref[2 + j]
            scale = jnp.broadcast_to(ratio[j : j + 1], (TILE, LANES))
            for k, slot in enumerate((owner, partner_of(owner, slot_count))):
                for t, (rows, lanes) in enumerate(tiles_of(row_count, half)):
                    at = slice(k * half + lanes.start, k * half + lanes.stop)
                    tile = slot_ref[slot, t].astype(jnp.float32)
                    out_ref[j, rows, at] = (scale * tile).astype(out_ref.dtype)
            if (j + 1) % per_piece == 0:
                piece = j // per_piece
                at = pl.ds(piece * per_piece, per_piece)
                copy = pltpu.make_async_copy(out_ref.at[at], out_any.at[at], sems.at[piece])
                copy.start()
                copies.append(copy)
        for copy in copies:
            copy.wait()

    return pl.pallas_call(
        body,
        out_shape=jax.ShapeDtypeStruct((blocks_here, row_count, 2 * half), slots.dtype),
        in_specs=[SMEM, VMEM],
        out_specs=ANY,
        scratch_shapes=[
            pltpu.VMEM((blocks_here, row_count, 2 * half), slots.dtype),
            pltpu.SemaphoreType.DMA((PIECES,)),
        ],
        compiler_params=params(4),
        name="scale_blocks",
    )(flags, slots)


def refresh(flags, grad_block, left_stats, right_stats):
    order = grad_block.shape[0]
    strip = 64

    def body(flag_ref, grad_ref, left_ref, right_ref, left_out, right_out, wide, low, first):
        def one(stat_ref, out_ref, dims):
            grad = grad_ref[...]
            wide[...] = lax.dot_general(grad, grad, dims, preferred_element_type=jnp.float32)

            def shift(i, total):
                at = pl.ds(i * strip, strip)
                on_diagonal = lax.broadcasted_iota(
                    jnp.int32, (strip, order), 1
                ) == i * strip + lax.broadcasted_iota(jnp.int32, (strip, order), 0)
                shifted = stat_decay * stat_ref[at] + wide[at] / order
                shifted = shifted + jnp.where(on_diagonal, ridge_term, 0.0)
                wide[at] = shifted
                return total + jnp.sum(
                    (shifted * shifted).reshape(strip // 8, 8, order), axis=0
                )

            squares = lax.fori_loop(
                0, order // strip, shift, jnp.zeros((8, order), jnp.float32)
            )
            scale = jnp.sqrt(jnp.sum(squares, keepdims=True) + tiny_term)
            start = 1.0 / jnp.sqrt(jnp.sqrt(scale))

            def begin(i, carry):
                at = pl.ds(i * strip, strip)
                on_diagonal = lax.broadcasted_iota(
                    jnp.int32, (strip, order), 1
                ) == i * strip + lax.broadcasted_iota(jnp.int32, (strip, order), 0)
                matrix = wide[at] / scale
                factor = ((jnp.where(on_diagonal, 5.0, 0.0) - matrix) / 4.0).astype(jnp.bfloat16)
                low[0, at] = matrix.astype(jnp.bfloat16)
                low[1, at] = factor
                first[at] = (start * factor.astype(jnp.float32)).astype(jnp.bfloat16)
                return carry

            lax.fori_loop(0, order // strip, begin, 0)

            def dot(a, b):
                return jnp.dot(a, b, preferred_element_type=jnp.float32)

            low[2] = dot(low[1], low[1]).astype(jnp.bfloat16)
            low[1] = dot(low[2], low[2]).astype(jnp.bfloat16)
            wide[...] = dot(low[1], low[0])

            def again(i, carry):
                at = pl.ds(i * strip, strip)
                on_diagonal = lax.broadcasted_iota(
                    jnp.int32, (strip, order), 1
                ) == i * strip + lax.broadcasted_iota(jnp.int32, (strip, order), 0)
                low[2, at] = ((jnp.where(on_diagonal, 5.0, 0.0) - wide[at]) / 4.0).astype(
                    jnp.bfloat16
                )
                return carry

            lax.fori_loop(0, order // strip, again, 0)
            out_ref[...] = dot(first[...], low[2]).astype(jnp.bfloat16)

        @pl.when(flag_ref[0] == 1)
        def _():
            one(left_ref, left_out, (((1,), (1,)), ((), ())))
            one(right_ref, right_out, (((0,), (0,)), ((), ())))

        @pl.when(flag_ref[0] == 0)
        def _():
            left_out[...] = jnp.zeros_like(left_out)
            right_out[...] = jnp.zeros_like(right_out)

    root = jax.ShapeDtypeStruct((order, order), jnp.bfloat16)
    return pl.pallas_call(
        body,
        out_shape=(root, root),
        in_specs=[SMEM, VMEM, VMEM, VMEM],
        out_specs=(VMEM, VMEM),
        scratch_shapes=[
            pltpu.VMEM((order, order), jnp.float32),
            pltpu.VMEM((3, order, order), jnp.bfloat16),
            pltpu.VMEM((order, order), jnp.bfloat16),
        ],
        compiler_params=params(24),
        name="refresh",
    )(flags, grad_block, left_stats, right_stats)


def shards(gradient, owners, left_stats, right_stats, left_roots_old, right_roots_old):
    dp_count = lax.axis_size(DP)
    mp_count = lax.axis_size(MP)
    blocks_here = gradient.shape[1]
    row_count = gradient.shape[2]
    block_width = gradient.shape[3]
    outgoing, flags = place_blocks(owners, gradient[0], dp_count)
    arrived = lax.all_to_all(outgoing, DP, split_axis=0, concat_axis=0, tiled=True)
    grad_block = arrived.reshape(dp_count * row_count, block_width)
    stays, passes, norms = precondition(
        flags, grad_block, left_roots_old[0, 0], right_roots_old[0, 0], blocks_here, mp_count, row_count
    )
    passed = lax.ppermute(passes, "dp_0h", [(0, 1), (1, 0)])
    row_norms = lax.all_to_all(norms, MP, split_axis=0, concat_axis=0, tiled=True)
    slots = fill_slots(flags, row_norms, passed, stays)
    returned = lax.all_to_all(slots, DP, split_axis=0, concat_axis=0, tiled=True)
    left_root, right_root = refresh(flags, grad_block, left_stats[0, 0], right_stats[0, 0])
    update = scale_blocks(flags, returned, row_count)[None]
    return (update, left_root[None, None], right_root[None, None])


def solution(mesh):
    finer = Mesh(
        mesh.devices.reshape(2, 2, 8, 2, 4, 2),
        ("dp_0h", "dp_0l", "dp_1", "dp_2", "mp_0", "mp_1"),
    )
    placed = (
        P(MP, None, DP, None),
        P(MP, None),
        P(MP, DP, None, None),
        P(MP, DP, None, None),
        P(MP, DP, None, None),
        P(MP, DP, None, None),
    )
    return jax.shard_map(
        shards,
        mesh=finer,
        in_specs=placed,
        out_specs=(P(MP, None, DP, None), P(MP, DP, None, None), P(MP, DP, None, None)),
        check_vma=False,
    )
```

```python
import jax
import jax.numpy as jnp
from jax import lax
from jax.experimental import pallas as pl
from jax.experimental.pallas import tpu as pltpu
from jax.sharding import Mesh
from jax.sharding import PartitionSpec as P

ITERS = 2
DP = ("dp_0h", "dp_0l", "dp_1", "dp_2")
MP = ("mp_0", "mp_1")
LANES = 128
TILE = 4
PIECES = 8
CHAINS = 8
MIB = 1024 * 1024
PLACE_MIB = 54


stat_decay = 0.9
ridge_term = 0.001
tiny_term = 1e-06

SMEM = pl.BlockSpec(memory_space=pltpu.SMEM)
VMEM = pl.BlockSpec(memory_space=pltpu.VMEM)
ANY = pl.BlockSpec(memory_space=pl.ANY)


def params(mib):
    return pltpu.CompilerParams(vmem_limit_bytes=mib * MIB)


def tiles_of(row_count, width):
    return [
        (slice(r, r + TILE), slice(c, c + LANES))
        for c in range(0, width, LANES)
        for r in range(0, row_count, TILE)
    ]


def partner_of(owner, dp_count):
    half = dp_count // 2
    return jnp.where(owner < half, owner + half, owner - half)


def place_blocks(owners, blocks, dp_count):
    blocks_here, row_count, width = blocks.shape
    per_piece = blocks_here // PIECES

    def body(owner_any, block_any, slot_ref, flag_ref, owner_ref, block_ref, sems):
        owner_fetch = pltpu.make_async_copy(owner_any, owner_ref, sems.at[PIECES])
        owner_fetch.start()
        fetches = []
        for piece in range(PIECES):
            at = pl.ds(piece * per_piece, per_piece)
            fetch = pltpu.make_async_copy(block_any.at[at], block_ref.at[at], sems.at[piece])
            fetch.start()
            fetches.append(fetch)
        owner_fetch.wait()
        my_index = lax.axis_index(DP)
        busy = jnp.int32(0)
        mine = jnp.int32(0)
        for j in range(blocks_here):
            if j % per_piece == 0:
                fetches[j // per_piece].wait()
            owner = owner_ref[0, j]
            rows = block_ref[j]
            slot_ref[owner] = rows
            slot_ref[partner_of(owner, dp_count)] = rows
            here = (owner == my_index).astype(jnp.int32)
            beside = (partner_of(owner, dp_count) == my_index).astype(jnp.int32)
            busy = busy + here
            mine = mine + (here + beside) * j
            flag_ref[2 + j] = owner
        flag_ref[0] = busy
        flag_ref[1] = mine

    return pl.pallas_call(
        body,
        out_shape=(
            pltpu.VMEM((dp_count, row_count, width), blocks.dtype),
            pltpu.SMEM((2 + blocks_here,), jnp.int32),
        ),
        in_specs=[ANY, ANY],
        out_specs=(VMEM, SMEM),
        scratch_shapes=[
            pltpu.SMEM(owners.shape, owners.dtype),
            pltpu.VMEM(blocks.shape, blocks.dtype),
            pltpu.SemaphoreType.DMA((PIECES + 1,)),
        ],
        compiler_params=params(PLACE_MIB),
        name="place_blocks",
    )(owners, blocks)


def precondition(flags, grad_block, left, right, blocks_here, mp_count, row_count):
    order = grad_block.shape[0]
    half = order // 2
    slots = order // row_count
    strip = 128

    def body(flag_ref, grad_ref, left_ref, right_ref, stay_ref, pass_ref, norm_ref):
        def squares_of(total, rows):
            wide = rows.astype(jnp.float32)
            return total + jnp.sum((wide * wide).reshape(strip // 8, 8, order), axis=0)

        def write_norm(lane_of, total):
            lane = lax.broadcasted_iota(jnp.int32, (1, LANES), 1)
            row = jnp.where(lane == lane_of, jnp.sum(total, keepdims=True), 0.0)
            norm_ref[...] = jnp.broadcast_to(row[None], norm_ref.shape)

        @pl.when(flag_ref[0] == 1)
        def _():
            shaded = jnp.dot(grad_ref[...], right_ref[...], preferred_element_type=jnp.float32)
            shaded = shaded.astype(jnp.bfloat16)
            total = jnp.zeros((8, order), jnp.float32)
            for i in range(order // strip):
                rows = jnp.dot(
                    left_ref[i * strip : (i + 1) * strip], shaded, preferred_element_type=jnp.float32
                ).astype(jnp.bfloat16)
                at = slice(i * strip // row_count, (i + 1) * strip // row_count)
                stay_ref[at] = rows[:, :half].reshape(strip // row_count, row_count, half)
                pass_ref[at] = rows[:, half:].reshape(strip // row_count, row_count, half)
                total = squares_of(total, rows)
            write_norm(flag_ref[1] + blocks_here, total)

        @pl.when(flag_ref[0] == 0)
        def _():
            total = jnp.zeros((8, order), jnp.float32)
            for i in range(order // strip):
                total = squares_of(total, grad_ref[i * strip : (i + 1) * strip])
            write_norm(flag_ref[1], total)

    return pl.pallas_call(
        body,
        out_shape=(
            pltpu.VMEM((slots, row_count, half), jnp.bfloat16),
            pltpu.VMEM((slots, row_count, half), jnp.bfloat16),
            pltpu.VMEM((mp_count, 1, LANES), jnp.float32),
        ),
        in_specs=[SMEM, VMEM, VMEM, VMEM],
        out_specs=(VMEM, VMEM, VMEM),
        compiler_params=params(12),
        name="precondition",
    )(flags, grad_block, left, right)


def fill_slots(flags, row_norms, passed, stays):
    slot_count, row_count, half = stays.shape
    tiles = row_count * half // (TILE * LANES)
    per_piece = slot_count // PIECES

    def body(flag_ref, norm_ref, passed_ref, stay_ref, out_any, out_ref, sems):
        total = jnp.sum(norm_ref[...], axis=0)
        high = total.astype(jnp.bfloat16).astype(jnp.float32)
        rest = total - high
        middle = rest.astype(jnp.bfloat16).astype(jnp.float32)
        low = rest - middle
        shape = (TILE, LANES)
        row = lax.broadcasted_iota(jnp.int32, shape, 0)
        packed = jnp.where(
            row == 0,
            jnp.broadcast_to(high, shape),
            jnp.where(
                row == 1,
                jnp.broadcast_to(middle, shape),
                jnp.where(row == 2, jnp.broadcast_to(low, shape), 0.0),
            ),
        ).astype(jnp.bfloat16)

        def fill(rows_ref):
            copies = []
            for piece in range(PIECES):
                at = pl.ds(piece * per_piece, per_piece)
                out_ref[at, tiles] = jnp.broadcast_to(packed[None], (per_piece, TILE, LANES))
                for t, (rows, lanes) in enumerate(tiles_of(row_count, half)):
                    out_ref[at, t] = rows_ref[at, rows, lanes]
                copy = pltpu.make_async_copy(out_ref.at[at], out_any.at[at], sems.at[piece])
                copy.start()
                copies.append(copy)
            for copy in copies:
                copy.wait()

        @pl.when(flag_ref[0] == 1)
        def _():
            fill(stay_ref)

        @pl.when(flag_ref[0] == 0)
        def _():
            fill(passed_ref)

    return pl.pallas_call(
        body,
        out_shape=jax.ShapeDtypeStruct((slot_count, tiles + 1, TILE, LANES), stays.dtype),
        in_specs=[SMEM, VMEM, VMEM, VMEM],
        out_specs=ANY,
        scratch_shapes=[
            pltpu.VMEM((slot_count, tiles + 1, TILE, LANES), stays.dtype),
            pltpu.SemaphoreType.DMA((PIECES,)),
        ],
        compiler_params=params(4),
        name="fill_slots",
    )(flags, row_norms, passed, stays)


def scale_blocks(flags, slots, row_count):
    blocks_here = flags.shape[0] - 2
    slot_count = slots.shape[0]
    tiles = slots.shape[1] - 1
    half = tiles * TILE * LANES // row_count
    per_piece = blocks_here // PIECES

    def body(flag_ref, slot_ref, out_any, out_ref, sems):
        copies = []
        chains = [slot_ref[p, tiles].astype(jnp.float32) for p in range(CHAINS)]
        for p in range(CHAINS, slot_count):
            chains[p % CHAINS] = chains[p % CHAINS] + slot_ref[p, tiles].astype(jnp.float32)
        while len(chains) > 1:
            chains = [one + two for one, two in zip(chains[::2], chains[1::2])]
        norms = chains[0]
        totals = norms[0:1] + (norms[1:2] + norms[2:3])
        columns = jnp.broadcast_to(totals, (LANES, LANES)).T
        ratio = jnp.sqrt(
            columns[:blocks_here] / (columns[blocks_here : 2 * blocks_here] + tiny_term)
        )
        for j in range(blocks_here):
            owner = flag_ref[2 + j]
            scale = jnp.broadcast_to(ratio[j : j + 1], (TILE, LANES))
            for k, slot in enumerate((owner, partner_of(owner, slot_count))):
                for t, (rows, lanes) in enumerate(tiles_of(row_count, half)):
                    at = slice(k * half + lanes.start, k * half + lanes.stop)
                    tile = slot_ref[slot, t].astype(jnp.float32)
                    out_ref[j, rows, at] = (scale * tile).astype(out_ref.dtype)
            if (j + 1) % per_piece == 0:
                piece = j // per_piece
                at = pl.ds(piece * per_piece, per_piece)
                copy = pltpu.make_async_copy(out_ref.at[at], out_any.at[at], sems.at[piece])
                copy.start()
                copies.append(copy)
        for copy in copies:
            copy.wait()

    return pl.pallas_call(
        body,
        out_shape=jax.ShapeDtypeStruct((blocks_here, row_count, 2 * half), slots.dtype),
        in_specs=[SMEM, VMEM],
        out_specs=ANY,
        scratch_shapes=[
            pltpu.VMEM((blocks_here, row_count, 2 * half), slots.dtype),
            pltpu.SemaphoreType.DMA((PIECES,)),
        ],
        compiler_params=params(4),
        name="scale_blocks",
    )(flags, slots)


def refresh(flags, grad_block, left_stats, right_stats):
    order = grad_block.shape[0]
    strip = 64

    def body(flag_ref, grad_ref, left_ref, right_ref, left_out, right_out, wide, low, first):
        def one(stat_ref, out_ref, dims):
            grad = grad_ref[...]
            wide[...] = lax.dot_general(grad, grad, dims, preferred_element_type=jnp.float32)

            def shift(i, total):
                at = pl.ds(i * strip, strip)
                on_diagonal = lax.broadcasted_iota(
                    jnp.int32, (strip, order), 1
                ) == i * strip + lax.broadcasted_iota(jnp.int32, (strip, order), 0)
                shifted = stat_decay * stat_ref[at] + wide[at] / order
                shifted = shifted + jnp.where(on_diagonal, ridge_term, 0.0)
                wide[at] = shifted
                return total + jnp.sum(
                    (shifted * shifted).reshape(strip // 8, 8, order), axis=0
                )

            squares = lax.fori_loop(
                0, order // strip, shift, jnp.zeros((8, order), jnp.float32)
            )
            scale = jnp.sqrt(jnp.sum(squares, keepdims=True) + tiny_term)
            start = 1.0 / jnp.sqrt(jnp.sqrt(scale))

            def begin(i, carry):
                at = pl.ds(i * strip, strip)
                on_diagonal = lax.broadcasted_iota(
                    jnp.int32, (strip, order), 1
                ) == i * strip + lax.broadcasted_iota(jnp.int32, (strip, order), 0)
                matrix = wide[at] / scale
                factor = ((jnp.where(on_diagonal, 5.0, 0.0) - matrix) / 4.0).astype(jnp.bfloat16)
                low[0, at] = matrix.astype(jnp.bfloat16)
                low[1, at] = factor
                first[at] = (start * factor.astype(jnp.float32)).astype(jnp.bfloat16)
                return carry

            lax.fori_loop(0, order // strip, begin, 0)

            def dot(a, b):
                return jnp.dot(a, b, preferred_element_type=jnp.float32)

            low[2] = dot(low[1], low[1]).astype(jnp.bfloat16)
            low[1] = dot(low[2], low[2]).astype(jnp.bfloat16)
            wide[...] = dot(low[1], low[0])

            def again(i, carry):
                at = pl.ds(i * strip, strip)
                on_diagonal = lax.broadcasted_iota(
                    jnp.int32, (strip, order), 1
                ) == i * strip + lax.broadcasted_iota(jnp.int32, (strip, order), 0)
                low[2, at] = ((jnp.where(on_diagonal, 5.0, 0.0) - wide[at]) / 4.0).astype(
                    jnp.bfloat16
                )
                return carry

            lax.fori_loop(0, order // strip, again, 0)
            out_ref[...] = dot(first[...], low[2]).astype(jnp.bfloat16)

        @pl.when(flag_ref[0] == 1)
        def _():
            one(left_ref, left_out, (((1,), (1,)), ((), ())))
            one(right_ref, right_out, (((0,), (0,)), ((), ())))

        @pl.when(flag_ref[0] == 0)
        def _():
            left_out[...] = jnp.zeros_like(left_out)
            right_out[...] = jnp.zeros_like(right_out)

    root = jax.ShapeDtypeStruct((order, order), jnp.bfloat16)
    return pl.pallas_call(
        body,
        out_shape=(root, root),
        in_specs=[SMEM, VMEM, VMEM, VMEM],
        out_specs=(VMEM, VMEM),
        scratch_shapes=[
            pltpu.VMEM((order, order), jnp.float32),
            pltpu.VMEM((3, order, order), jnp.bfloat16),
            pltpu.VMEM((order, order), jnp.bfloat16),
        ],
        compiler_params=params(24),
        name="refresh",
    )(flags, grad_block, left_stats, right_stats)


def shards(gradient, owners, left_stats, right_stats, left_roots_old, right_roots_old):
    dp_count = lax.axis_size(DP)
    mp_count = lax.axis_size(MP)
    blocks_here = gradient.shape[1]
    row_count = gradient.shape[2]
    block_width = gradient.shape[3]
    outgoing, flags = place_blocks(owners, gradient[0], dp_count)
    arrived = lax.all_to_all(outgoing, DP, split_axis=0, concat_axis=0, tiled=True)
    grad_block = arrived.reshape(dp_count * row_count, block_width)
    stays, passes, norms = precondition(
        flags, grad_block, left_roots_old[0, 0], right_roots_old[0, 0], blocks_here, mp_count, row_count
    )
    passed = lax.ppermute(passes, "dp_0h", [(0, 1), (1, 0)])
    row_norms = lax.all_to_all(norms, MP, split_axis=0, concat_axis=0, tiled=True)
    slots = fill_slots(flags, row_norms, passed, stays)
    returned = lax.all_to_all(slots, DP, split_axis=0, concat_axis=0, tiled=True)
    left_root, right_root = refresh(flags, grad_block, left_stats[0, 0], right_stats[0, 0])
    update = scale_blocks(flags, returned, row_count)[None]
    return (update, left_root[None, None], right_root[None, None])


def solution(mesh):
    finer = Mesh(
        mesh.devices.reshape(2, 2, 8, 2, 4, 2),
        ("dp_0h", "dp_0l", "dp_1", "dp_2", "mp_0", "mp_1"),
    )
    placed = (
        P(MP, None, DP, None),
        P(MP, None),
        P(MP, DP, None, None),
        P(MP, DP, None, None),
        P(MP, DP, None, None),
        P(MP, DP, None, None),
    )
    return jax.shard_map(
        shards,
        mesh=finer,
        in_specs=placed,
        out_specs=(P(MP, None, DP, None), P(MP, DP, None, None), P(MP, DP, None, None)),
        check_vma=False,
    )
```
